256 devices in a mesh: blk: 4 (over y), py: 8 (over z), pz: 8 (over x, core).
Axes of the slice: x: 4, y: 4, z: 8, core: 2. Of those that a mesh axis runs over, the one named last changes fastest.
Arguments:
- source: float32 [256, 1024, 128], P(('py', 'pz'), 'blk'), may hold values from -6 to 6
- conduct: float32 [3], replicated, may hold values from 0.3 to 3
- neighbours: int32 [4, 2], replicated, may hold values from -1 to 3, as said below
- orient: int32 [4], replicated, may hold values 0 or 1
Outputs:
- solution: float32 [256, 1024, 128], P(('py', 'pz'), 'blk')
- norms: float32 [3], replicated
The draws below stay inside these ranges and needn't reach their ends.
Inputs may be any that keep to these rules, and one draw needn't show every extreme that they name: `neighbours`: the blocks form one chain: row b holds the left and the right neighbour of block b, -1 marks the two ends, and a block is the left neighbour of its right neighbour.
All inputs are finite; a program needn't handle non-finite values.
Results may differ from the reference program's by a relative error of at most 0.00011.
Values sent between devices are 32-bit elements; how exact they have to be, the bound alone decides.
A program may use at most 64 MiB of HBM per device.

```python
import math
import jax
import jax.numpy as jnp
from jax import lax

NY = 256
NZ = 128
BX = 256
OV = 64
ITERS = 3
EXT = 384
BLOCKS = 4
CHAIN = 1024


def draw_neighbours(key, part):
    own_key = jax.random.fold_in(key, 7919)
    scores = jax.random.randint(own_key, (BLOCKS,), 0, 1073741824, dtype=jnp.int32)
    block_ids = jnp.arange(BLOCKS, dtype=jnp.int32)
    before = (scores[None, :] < scores[:, None]) | (scores[None, :] == scores[:, None]) & (block_ids[None, :] < block_ids[:, None])
    position = jnp.sum(before.astype(jnp.int32), axis=1).astype(jnp.int32)
    prev_match = position[None, :] == (position - 1)[:, None]
    next_match = position[None, :] == (position + 1)[:, None]
    previous_id = jnp.sum(jnp.where(prev_match, block_ids[None, :], 0), axis=1).astype(jnp.int32)
    following_id = jnp.sum(jnp.where(next_match, block_ids[None, :], 0), axis=1).astype(jnp.int32)
    previous = jnp.where(position > 0, previous_id, -1)
    following = jnp.where(position < BLOCKS - 1, following_id, -1)
    return jnp.stack([previous, following], axis=1).astype(jnp.int32)


def place_ends(values, rng, low, high):
    extent = values.shape
    place = [jax.random.randint(jax.random.fold_in(rng, axis), (), 0, extent[axis]) for axis in range(len(extent))]
    values = values.at[tuple(place)].set(low)
    longest = extent.index(max(extent))
    place[longest] = (place[longest] + 1) % extent[longest]
    return values.at[tuple(place)].set(high)


def shard_levels(key, dims, split, low, high):
    def one(dim, parts):
        heights = jax.random.uniform(jax.random.fold_in(jax.random.fold_in(key, 6), dim), (parts,), jnp.float32, low / len(split), high / len(split))
        return jnp.repeat(jnp.exp(heights), dims[dim] // parts).reshape((-1,) + (1,) * (len(dims) - dim - 1))

    gain = one(*split[0])
    for cut in split[1:]:
        gain = gain * one(*cut)
    return gain


def gaussian(key, dims, width, reach, cuts=(), kind=jnp.bfloat16):
    array = width * jax.random.normal(key, dims, jnp.float32)
    if cuts:
        array = array * shard_levels(key, dims, cuts, -0.22, 0.18)
    return jnp.clip(array, -reach, reach).astype(kind)


def setup_inputs(seed: int = 0) -> dict:
    splits = jax.random.split(jax.random.key(seed), 5)
    source = gaussian(splits[0], (NY, CHAIN, NZ), 1.0, 6.0, ((0, 64), (1, 4)), jnp.float32)
    conduct = jnp.clip(jnp.exp(jax.random.uniform(splits[1], (3,), jnp.float32, math.log(0.3), math.log(3.0))), 0.3, 3.0)
    neighbours = draw_neighbours(jax.random.fold_in(splits[4], 71), 0)
    orient = place_ends((jax.random.randint(splits[3], (BLOCKS,), 0, 2) < 1).astype(jnp.int32), jax.random.fold_in(splits[3], 1), 0, 1)
    return dict(source=source, conduct=conduct, neighbours=neighbours, orient=orient)


HIGHEST = lax.Precision.HIGHEST

def sine_basis(row_index, col_index, length):
    product = (row_index[:, None] + 1) * (col_index[None, :] + 1) % (2 * (length + 1))
    angles = jnp.pi * product.astype(jnp.float32) / (length + 1)
    return (jnp.sqrt(2.0 / (length + 1)) * jnp.sin(angles)).astype(jnp.float32)

def spectrum(index, length):
    angles = jnp.pi * (index.astype(jnp.float32) + 1.0) / (2.0 * (length + 1))
    return (4.0 * jnp.sin(angles) ** 2).astype(jnp.float32)

def apply_operator(extended, conduct):
    centre = extended[:, 1:-1, :]
    padded = jnp.pad(centre, ((1, 1), (0, 0), (1, 1)))
    along = 2.0 * centre - extended[:, :-2, :] - extended[:, 2:, :]
    across = 2.0 * centre - padded[:-2, :, 1:-1] - padded[2:, :, 1:-1]
    depth = 2.0 * centre - padded[1:-1, :, :-2] - padded[1:-1, :, 2:]
    return conduct[0] * along + conduct[1] * across + conduct[2] * depth

def block_solve(residual, plane_basis, row_basis, depth_basis, spectra):
    modes = jnp.einsum('yxz,xk->ykz', residual, plane_basis, precision=HIGHEST)
    modes = jnp.einsum('yxz,yk->kxz', modes, row_basis, precision=HIGHEST)
    modes = jnp.einsum('yxz,zk->yxk', modes, depth_basis, precision=HIGHEST)
    modes = modes / spectra
    modes = jnp.einsum('yxz,zk->yxk', modes, depth_basis, precision=HIGHEST)
    modes = jnp.einsum('kxz,yk->yxz', modes, row_basis, precision=HIGHEST)
    return jnp.einsum('ykz,xk->yxz', modes, plane_basis, precision=HIGHEST)

def reference(source, conduct, neighbours, orient):
    blocks = neighbours.shape[0]
    plane_ids = jnp.arange(EXT, dtype=jnp.int32)
    row_ids = jnp.arange(NY, dtype=jnp.int32)
    depth_ids = jnp.arange(NZ, dtype=jnp.int32)
    plane_basis = sine_basis(plane_ids, plane_ids, EXT)
    row_basis = sine_basis(row_ids, row_ids, NY)
    depth_basis = sine_basis(depth_ids, depth_ids, NZ)
    spectra = conduct[0] * spectrum(plane_ids, EXT)[None, :, None] + conduct[1] * spectrum(row_ids, NY)[:, None, None] + conduct[2] * spectrum(depth_ids, NZ)[None, None, :]
    sources = []
    for block in range(blocks):
        piece = source[:, block * BX:(block + 1) * BX, :]
        sources.append(jnp.where(orient[block] == 1, piece[:, ::-1, :], piece))
    source_stack = jnp.stack(sources)
    iterates = [jnp.zeros((NY, BX, NZ), jnp.float32) for block in range(blocks)]
    plane_pos = jnp.arange(EXT, dtype=jnp.int32)
    cell_count = float(blocks * BX * NY * NZ)
    norm_list = []
    for iteration in range(ITERS):
        iterate_stack = jnp.stack(iterates)
        updated = []
        squares = jnp.zeros((), jnp.float32)
        for block in range(blocks):
            left_id = neighbours[block, 0]
            right_id = neighbours[block, 1]
            has_left = (left_id >= 0).astype(jnp.float32)
            has_right = (right_id >= 0).astype(jnp.float32)
            left_safe = jnp.maximum(left_id, 0)
            right_safe = jnp.maximum(right_id, 0)
            extended = jnp.concatenate([iterate_stack[left_safe][:, BX - OV - 1:, :] * has_left, iterates[block], iterate_stack[right_safe][:, :OV + 1, :] * has_right], axis=1)
            source_ext = jnp.concatenate([source_stack[left_safe][:, BX - OV:, :] * has_left, sources[block], source_stack[right_safe][:, :OV, :] * has_right], axis=1)
            plane_mask = jnp.where(plane_pos < OV, has_left, jnp.where(plane_pos >= OV + BX, has_right, 1.0))
            residual = (source_ext - apply_operator(extended, conduct)) * plane_mask[None, :, None]
            squares = squares + jnp.sum(residual[:, OV:OV + BX, :] ** 2)
            correction = block_solve(residual, plane_basis, row_basis, depth_basis, spectra)
            updated.append(iterates[block] + correction[:, OV:OV + BX, :])
        norm_list.append(jnp.sqrt(squares / cell_count))
        iterates = updated
    placed = [jnp.where(orient[block] == 1, iterates[block][:, ::-1, :], iterates[block]) for block in range(blocks)]
    return (jnp.concatenate(placed, axis=1), jnp.stack(norm_list).astype(jnp.float32))
```

```python
import functools

import jax
import jax.numpy as jnp
import ml_dtypes
import numpy as np
from jax import lax
from jax.experimental import pallas as pl
from jax.experimental.pallas import tpu as pltpu
from jax.sharding import PartitionSpec as P

NY = 256
NZ = 128
BX = 256
OV = 64
EXT = 384
BLOCKS = 4
PY = 8
PZ = 8
PLANE = PY * PZ
ROWS = NY // PLANE
HALVES = 2
MODES = 256
MESH = pl.DeviceIdType.MESH
F32 = jnp.float32
BF16 = jnp.bfloat16
NN = (((1,), (0,)), ((), ()))
NT = (((1,), (1,)), ((), ()))
CELLS = float(BLOCKS * BX * NY * NZ)


def basis(n):
    j = np.arange(1, n + 1)
    m = (j[:, None] * j[None, :]) % (2 * (n + 1))
    return np.sqrt(2.0 / (n + 1)) * np.sin(np.pi * m / (n + 1))


def eigenvalues(n):
    return 4.0 * np.sin(np.pi * np.arange(1, n + 1) / (2.0 * (n + 1))) ** 2


def halves(a):
    a = a.astype(np.float32)
    hi = a.astype(ml_dtypes.bfloat16)
    lo = (a - hi.astype(np.float32)).astype(ml_dtypes.bfloat16)
    return np.stack([hi, lo])


@functools.lru_cache(None)
def tables():
    depth = basis(NZ)
    rows = basis(NY)
    planes = basis(EXT)
    margin = basis(OV)
    order = (ROWS * np.arange(PLANE)[None, :] + np.arange(ROWS)[:, None]).reshape(-1)
    rows_in = rows[:, order]
    ends = np.zeros((2 * OV, BX))
    ends[:OV, :OV] = margin[0][:, None] * margin.T
    ends[OV:, BX - OV :] = margin[OV - 1][:, None] * margin.T
    planes_in = planes[OV : OV + BX].T
    four = np.zeros((8, EXT))
    four[:4] = planes[[OV - 1, OV, OV + BX - 1, OV + BX]]
    lanes = np.ones((1, 128))
    return (
        halves(depth),
        halves(rows_in),
        halves(rows_in.T),
        halves(np.concatenate([planes_in, ends], axis=0)),
        halves(planes_in.T),
        halves(four),
        halves(four.T),
        (eigenvalues(EXT)[:, None] * lanes).astype(np.float32),
        (eigenvalues(OV)[:, None] * lanes).astype(np.float32),
        eigenvalues(NY)[None, :].astype(np.float32),
    )


def split(x):
    hi = x.astype(BF16)
    return hi, (x - hi.astype(F32)).astype(BF16)


def times(table, x, dims):
    hi, lo = split(x)
    dot = functools.partial(lax.dot_general, dimension_numbers=dims, preferred_element_type=F32)
    return dot(table[0], hi) + (dot(table[0], lo) + dot(table[1], hi))


def times_right(x, table, dims):
    hi, lo = split(x)
    dot = functools.partial(lax.dot_general, dimension_numbers=dims, preferred_element_type=F32)
    return dot(hi, table[0]) + (dot(lo, table[0]) + dot(hi, table[1]))


def kernel(
    source,
    conduct,
    neighbours,
    orient,
    depth_spectrum,
    *refs,
):
    consts_hbm = refs[:10]
    out, norms = refs[10:12]
    consts = refs[12:22]
    (
        src,
        sent,
        got,
        modes,
        inverse,
        inverse_margin,
        ends_out,
        ends_in,
        back,
        returned,
        result,
        norm_out,
        norm_x,
        norm_mid,
        norm_z,
        src_sem,
        const_sem,
        out_sem,
        go_send,
        go_recv,
        ends_send,
        ends_recv,
        back_send,
        back_recv,
        norm_send,
        norm_recv,
    ) = refs[22:]
    depth, rows_in, rows_out, planes_in, planes_out, four_in, four_out, mu_planes, mu_margin, mu_rows = consts

    blk = lax.axis_index("blk")
    py = lax.axis_index("py")
    pz = lax.axis_index("pz")
    place = py * PZ + pz

    def peer(step):
        to_py = lax.rem(py + lax.rem(step, PY), PY)
        to_pz = lax.rem(pz + step // PY, PZ)
        return to_py, to_pz, to_py * PZ + to_pz

    barrier = pltpu.get_barrier_semaphore()

    def greet(step, carry):
        to_py, to_pz, _ = peer(step)
        pl.semaphore_signal(barrier, inc=1, device_id=(blk, to_py, to_pz), device_id_type=MESH)
        return carry

    loads = [pltpu.make_async_copy(source.at[y], src.at[y], src_sem.at[y]) for y in range(ROWS)]
    fetches = [pltpu.make_async_copy(a, b, const_sem.at[i]) for i, (a, b) in enumerate(zip(consts_hbm, consts))]
    fetches[0].start()
    for load in loads:
        load.start()
    lax.fori_loop(1, PLANE, greet, 0)
    for step in range(1, BLOCKS):
        pl.semaphore_signal(
            barrier, inc=1, device_id=(lax.rem(blk + step, BLOCKS), py, pz), device_id_type=MESH
        )
    for fetch in fetches[1:]:
        fetch.start()

    fetches[0].wait()
    squares = jnp.zeros((8, 128), F32)
    for y in range(ROWS):
        loads[y].wait()
        cells = src[y]
        squares = squares + jnp.sum((cells * cells).reshape(BX // 8, 8, NZ), axis=0)
        z = times((depth[0], depth[1]), cells, NT)
        for h in range(HALVES):
            for x in range(2):
                sent[h, pl.ds(4 * x + y, PLANE, stride=8), :] = z[
                    PLANE * h : PLANE * (h + 1), 128 * x : 128 * (x + 1)
                ]
    own_squares = jnp.sum(jnp.sum(squares, axis=0, keepdims=True), axis=1, keepdims=True)

    pl.semaphore_wait(barrier, PLANE - 1 + BLOCKS - 1)

    def tile(d):
        return pl.ds(pl.multiple_of(d * 8, 8), 8)

    def exchange(src_ref, dst_ref, send_sem, recv_sem, h):
        def send(step, carry):
            to_py, to_pz, to = peer(step)
            pltpu.make_async_remote_copy(
                src_ref=src_ref.at[h, tile(to), :],
                dst_ref=dst_ref.at[h, tile(place), :],
                send_sem=send_sem.at[h],
                recv_sem=recv_sem.at[h],
                device_id=(blk, to_py, to_pz),
                device_id_type=MESH,
            ).start()
            return carry

        lax.fori_loop(1, PLANE, send, 0)
        dst_ref[h, tile(place), :] = src_ref[h, tile(place), :]

    def all_of(src_ref, dst_ref, send_sem, recv_sem, h):
        others = pl.ds(0, (PLANE - 1) * 8)
        return pltpu.make_async_remote_copy(
            src_ref=src_ref.at[h, others, :],
            dst_ref=dst_ref.at[h, others, :],
            send_sem=send_sem.at[h],
            recv_sem=recv_sem.at[h],
            device_id=(blk, lax.rem(py + 1, PY), pz),
            device_id_type=MESH,
        )

    for h in range(HALVES):
        exchange(sent, got, go_send, go_recv, h)

    for fetch in fetches[1:]:
        fetch.wait()

    c0 = conduct[0]
    c1 = conduct[1]
    c2 = conduct[2]

    order = [jnp.int32(0)]
    for b in range(BLOCKS):
        order[0] = order[0] + b * (neighbours[b, 0] == -1).astype(jnp.int32)
    for m in range(1, BLOCKS):
        following = jnp.int32(0)
        for b in range(BLOCKS):
            following = following + neighbours[b, 1] * (order[m - 1] == b).astype(jnp.int32)
        order.append(following)
    is_at = [[(order[m] == b).astype(F32) for b in range(BLOCKS)] for m in range(BLOCKS)]
    own_at = [(order[m] == blk).astype(F32) for m in range(BLOCKS)]
    block_flips = [(orient[b] == 1).astype(F32) for b in range(BLOCKS)]
    flips = [sum(is_at[m][b] * block_flips[b] for b in range(BLOCKS)) for m in range(BLOCKS)]
    own_flip = sum(own_at[m] * flips[m] for m in range(BLOCKS))

    row_id = lax.broadcasted_iota(jnp.int32, (8, MODES), 0)

    def pick(flag, yes, no):
        return yes * flag + no * (1.0 - flag)

    greens = []
    for h in range(HALVES):
        shift = c1 * mu_rows[...] + c2 * depth_spectrum[PLANE * h + place]
        inverse[h] = 1.0 / (c0 * jnp.concatenate([mu_planes[...]] * 2, axis=1) + shift)
        inverse_margin[h] = 1.0 / (c0 * jnp.concatenate([mu_margin[...]] * 2, axis=1) + shift)
        half = jnp.sqrt(shift / (4.0 * c0))
        square = half * half
        theta = 2.0 * jnp.log1p(half + square / (1.0 + jnp.sqrt(1.0 + square)))

        def power(n):
            return jnp.exp(-n * theta)

        def fall(n):
            return 1.0 - power(2.0 * n)

        scale = 1.0 / (fall(1.0) * fall(385.0))
        f64, f65, f320, f321 = fall(64.0), fall(65.0), fall(320.0), fall(321.0)
        table = {
            (0, 0): power(1.0) * f64 * f321 * scale,
            (0, 1): power(2.0) * f64 * f320 * scale,
            (0, 2): power(257.0) * f64 * f65 * scale,
            (0, 3): power(258.0) * f64 * f64 * scale,
            (1, 1): power(1.0) * f65 * f320 * scale,
            (1, 2): power(256.0) * f65 * f65 * scale,
        }
        for a, b, c, d in ((1, 3, 0, 2), (2, 2, 1, 1), (2, 3, 0, 1), (3, 3, 0, 0)):
            table[a, b] = table[c, d]
        for a in range(4):
            for b in range(a):
                table[a, b] = table[b, a]
        greens.append((table, jnp.exp(theta) * f65 / f64))

    def to_ends(h, step):
        return pltpu.make_async_remote_copy(
            src_ref=ends_out.at[h],
            dst_ref=ends_in.at[h, blk],
            send_sem=ends_send.at[h, step - 1],
            recv_sem=ends_recv.at[h, step - 1],
            device_id=(lax.rem(blk + step, BLOCKS), py, pz),
            device_id_type=MESH,
        )

    def assembled(ref, h, r):
        return jnp.concatenate(
            [ref[h, pl.ds(4 * x + r, PLANE, stride=8), :] for x in range(2)], axis=1
        )

    for h in range(HALVES):
        all_of(sent, got, go_send, go_recv, h).wait_recv()
        plane = jnp.concatenate([assembled(got, h, r) for r in range(ROWS)], axis=0)
        hat = times((rows_in[0], rows_in[1]), plane, NN)
        both = times((planes_in[0], planes_in[1]), hat, NT)
        held = both[:EXT]
        modes[h] = held
        near = times((four_in[0], four_in[1]), held * inverse[h], NN)
        margins = both[EXT:]
        ratio = greens[h][1]
        low = jnp.sum(margins[:OV] * inverse_margin[h], axis=0, keepdims=True) * ratio
        high = jnp.sum(margins[OV:] * inverse_margin[h], axis=0, keepdims=True) * ratio
        near = (
            near
            + jnp.where(row_id == 4, low, 0.0)
            + jnp.where(row_id == 5, high, 0.0)
            + jnp.where(row_id == 6, own_squares, 0.0)
        )
        ends_out[h] = near
        ends_in[h, blk] = near
        for step in range(1, BLOCKS):
            to_ends(h, step).start()

    change_1 = jnp.zeros((1, MODES), F32)
    change_2 = jnp.zeros((1, MODES), F32)
    total_squares = jnp.zeros((1, 1), F32)
    for h in range(HALVES):
        for step in range(1, BLOCKS):
            to_ends(h, step).wait_recv()
        table = greens[h][0]
        tiles = [ends_in[h, b] for b in range(BLOCKS)]
        if h == 0:
            for b in range(BLOCKS):
                total_squares = total_squares + tiles[b][6:7, :1]
        base, low, high = [], [], []
        for m in range(BLOCKS):
            at = sum(tiles[b] * is_at[m][b] for b in range(BLOCKS))
            row = [at[i : i + 1] for i in range(6)]
            base.append([pick(flips[m], row[3 - p], row[p]) for p in range(4)])
            low.append(pick(flips[m], row[5], row[4]))
            high.append(pick(flips[m], row[4], row[5]))
        zero = jnp.zeros((1, MODES), F32)
        outer = [
            [high[m - 1] if m > 0 else zero, zero, zero, low[m + 1] if m < BLOCKS - 1 else zero]
            for m in range(BLOCKS)
        ]

        def solved(m, p, sources):
            return base[m][p] + sum(table[p, q] * sources[m][q] for q in range(4))

        def jumps(sources):
            last = BLOCKS - 1
            left = [solved(m + 1, 1, sources) - solved(m, 3, sources) for m in range(last)]
            left.append(-solved(last, 3, sources))
            right = [solved(m, 2, sources) - solved(m + 1, 0, sources) for m in range(last)]
            right.append(-solved(0, 0, sources))
            return left, right

        def with_jumps(left, right):
            result = [list(o) for o in outer]
            for m in range(BLOCKS - 1):
                result[m][2] = left[m]
                result[m][3] = outer[m][3] + right[m]
                result[m + 1][1] = right[m]
                result[m + 1][0] = outer[m + 1][0] + left[m]
            result[BLOCKS - 1][2] = left[BLOCKS - 1]
            result[0][1] = right[BLOCKS - 1]
            return result

        left_1, right_1 = jumps(outer)
        left_2, right_2 = jumps(with_jumps(left_1, right_1))
        for a, b in zip(left_1 + right_1, left_2 + right_2):
            change_1 = change_1 + a * a
            change_2 = change_2 + (b - a) * (b - a)
        final = with_jumps(left_2, right_2)
        own = [sum(own_at[m] * final[m][p] for m in range(BLOCKS)) for p in range(4)]
        own = [pick(own_flip, own[3 - p], own[p]) for p in range(4)]
        added = sum(jnp.where(row_id == p, own[p] * c0, 0.0) for p in range(4))
        solution_modes = inverse[h] * (modes[h] + times((four_out[0], four_out[1]), added, NN))
        across = times((planes_out[0], planes_out[1]), solution_modes, NN)
        plane = times((rows_out[0], rows_out[1]), across, NT)
        for r in range(ROWS):
            for x in range(2):
                back[h, pl.ds(4 * x + r, PLANE, stride=8), :] = plane[
                    PLANE * r : PLANE * (r + 1), 128 * x : 128 * (x + 1)
                ]
        exchange(back, returned, back_send, back_recv, h)

    lane = lax.broadcasted_iota(jnp.int32, (1, 128), 1)

    def total(x):
        return jnp.sum(x, axis=1, keepdims=True)

    partial = (
        jnp.where(lane == 0, total_squares, 0.0)
        + jnp.where(lane == 1, total(change_1) * (c0 * c0), 0.0)
        + jnp.where(lane == 2, total(change_2) * (c0 * c0), 0.0)
    )

    def norm_copy(src_ref, dst_ref, stage, step):
        device = (
            (blk, py, lax.rem(pz + step, PZ)) if stage == 0 else (blk, lax.rem(py + step, PY), pz)
        )
        return pltpu.make_async_remote_copy(
            src_ref=src_ref,
            dst_ref=dst_ref.at[pz if stage == 0 else py],
            send_sem=norm_send.at[stage, step - 1],
            recv_sem=norm_recv.at[stage, step - 1],
            device_id=device,
            device_id_type=MESH,
        )

    norm_out[...] = partial
    norm_x[pz] = partial
    for step in range(1, PZ):
        norm_copy(norm_out, norm_x, 0, step).start()
    for step in range(1, PZ):
        norm_copy(norm_out, norm_x, 0, step).wait_recv()
    partial = sum(norm_x[i] for i in range(PZ))
    norm_mid[...] = partial
    norm_z[py] = partial
    for step in range(1, PY):
        norm_copy(norm_mid, norm_z, 1, step).start()

    for h in range(HALVES):
        all_of(back, returned, back_send, back_recv, h).wait_recv()
    for r in range(ROWS):
        stacked = jnp.concatenate([assembled(returned, h, r) for h in range(HALVES)], axis=0)
        result[r] = times_right(stacked.T, (depth[0], depth[1]), NN)
        pltpu.make_async_copy(result.at[r], out.at[r], out_sem.at[r]).start()

    for step in range(1, PY):
        norm_copy(norm_mid, norm_z, 1, step).wait_recv()
    partial = jnp.sqrt(sum(norm_z[i] for i in range(PY)) / CELLS)
    for i in range(3):
        norms[i] = jnp.sum(jnp.where(lane == i, partial, 0.0))

    for h in range(HALVES):
        all_of(sent, got, go_send, go_recv, h).wait_send()
        all_of(back, returned, back_send, back_recv, h).wait_send()
        for step in range(1, BLOCKS):
            to_ends(h, step).wait_send()
    for step in range(1, PZ):
        norm_copy(norm_out, norm_x, 0, step).wait_send()
        norm_copy(norm_mid, norm_z, 1, step).wait_send()
    for r in range(ROWS):
        pltpu.make_async_copy(result.at[r], out.at[r], out_sem.at[r]).wait()


def shards(source, conduct, neighbours, orient):
    consts = tables()
    any_space = pl.BlockSpec(memory_space=pl.ANY)
    smem = pl.BlockSpec(memory_space=pltpu.SMEM)
    dma = pltpu.SemaphoreType.DMA
    chunked = pltpu.VMEM((HALVES, PLANE * 8, 128), F32)
    return pl.pallas_call(
        kernel,
        name="schwarz",
        out_shape=(
            jax.ShapeDtypeStruct((ROWS, BX, NZ), F32),
            jax.ShapeDtypeStruct((3,), F32),
        ),
        in_specs=[any_space, smem, smem, smem, smem] + [any_space] * len(consts),
        out_specs=(any_space, smem),
        scratch_shapes=[pltpu.VMEM(c.shape, c.dtype) for c in consts]
        + [
            pltpu.VMEM((ROWS, BX, NZ), F32),
            chunked,
            chunked,
            pltpu.VMEM((HALVES, EXT, MODES), F32),
            pltpu.VMEM((HALVES, EXT, MODES), F32),
            pltpu.VMEM((HALVES, OV, MODES), F32),
            pltpu.VMEM((HALVES, 8, MODES), F32),
            pltpu.VMEM((HALVES, BLOCKS, 8, MODES), F32),
            chunked,
            chunked,
            pltpu.VMEM((ROWS, BX, NZ), F32),
            pltpu.VMEM((1, 128), F32),
            pltpu.VMEM((PZ, 1, 128), F32),
            pltpu.VMEM((1, 128), F32),
            pltpu.VMEM((PY, 1, 128), F32),
            dma((ROWS,)),
            dma((len(consts),)),
            dma((ROWS,)),
            dma((HALVES,)),
            dma((HALVES,)),
            dma((HALVES, BLOCKS - 1)),
            dma((HALVES, BLOCKS - 1)),
            dma((HALVES,)),
            dma((HALVES,)),
            dma((2, PZ - 1)),
            dma((2, PZ - 1)),
        ],
        compiler_params=pltpu.CompilerParams(collective_id=0, has_side_effects=True),
    )(
        source,
        conduct,
        neighbours,
        orient,
        jnp.asarray(eigenvalues(NZ).astype(np.float32)),
        *[jnp.asarray(c) for c in consts],
    )


def solution(mesh):
    cells = P(("py", "pz"), "blk", None)
    return jax.shard_map(
        shards, mesh=mesh, in_specs=(cells, P(), P(), P()), out_specs=(cells, P()), check_vma=False
    )
```

```python
import functools

import jax
import jax.numpy as jnp
import ml_dtypes
import numpy as np
from jax import lax
from jax.experimental import pallas as pl
from jax.experimental.pallas import tpu as pltpu
from jax.sharding import PartitionSpec as P

NY = 256
NZ = 128
BX = 256
OV = 64
EXT = 384
BLOCKS = 4
PY = 8
PZ = 8
PLANE = PY * PZ
ROWS = NY // PLANE
HALVES = 2
MODES = 256
MESH = pl.DeviceIdType.MESH
F32 = jnp.float32
BF16 = jnp.bfloat16
NN = (((1,), (0,)), ((), ()))
NT = (((1,), (1,)), ((), ()))
CELLS = float(BLOCKS * BX * NY * NZ)
TN = (((0,), (0,)), ((), ()))


def basis(n):
    j = np.arange(1, n + 1)
    m = (j[:, None] * j[None, :]) % (2 * (n + 1))
    return np.sqrt(2.0 / (n + 1)) * np.sin(np.pi * m / (n + 1))


def eigenvalues(n):
    return 4.0 * np.sin(np.pi * np.arange(1, n + 1) / (2.0 * (n + 1))) ** 2


def halves(a):
    a = a.astype(np.float32)
    hi = a.astype(ml_dtypes.bfloat16)
    lo = (a - hi.astype(np.float32)).astype(ml_dtypes.bfloat16)
    return np.stack([hi, lo])


@functools.lru_cache(None)
def tables():
    depth = halves(basis(NZ))
    rows = basis(NY)
    planes = basis(EXT)
    order = (ROWS * np.arange(PLANE)[None, :] + np.arange(ROWS)[:, None]).reshape(-1)
    planes_in = planes[OV : OV + BX].T
    depth_in = np.concatenate([depth[0], depth[0], depth[1]], axis=1)
    depth_out = np.stack(
        [
            np.concatenate([part[PLANE * h : PLANE * (h + 1)] for part in (depth[0], depth[0], depth[1])], axis=0)
            for h in range(HALVES)
        ]
    )
    return (
        depth_in,
        halves(rows[order]),
        halves(rows[order]),
        halves(planes_in),
        halves(planes_in.T),
        (eigenvalues(EXT)[:, None] * np.ones((1, 128))).astype(np.float32),
        eigenvalues(NY)[None, :].astype(np.float32),
        depth_out,
    )


def split(x):
    hi = x.astype(BF16)
    return hi, (x - hi.astype(F32)).astype(BF16)


def dot(a, b, dims):
    return lax.dot_general(a, b, dimension_numbers=dims, preferred_element_type=F32)


def times(table, x, dims):
    hi, lo = split(x)
    return dot(table[0], hi, dims) + (dot(table[0], lo, dims) + dot(table[1], hi, dims))


def times_right(x, table, dims):
    hi, lo = split(x)
    return dot(hi, table[0], dims) + (dot(lo, table[0], dims) + dot(hi, table[1], dims))


def assembled(ref, h, r):
    return jnp.concatenate([ref[h, pl.ds(4 * x + r, PLANE, stride=8), :] for x in range(2)], axis=1)


def depth_back(ref, h, r, table):
    hi, lo = split(assembled(ref, h, r))
    return dot(jnp.concatenate([hi, lo, hi], axis=0), table[h], TN)


def kernel(source, conduct_hbm, neighbours_hbm, orient_hbm, spectrum_hbm, *refs):
    consts_hbm = refs[:8]
    returned, partial_out, norm_z, depth_out = refs[8:12]
    consts = refs[12:19] + (depth_out,)
    (
        conduct,
        neighbours,
        orient,
        depth_spectrum,
        src,
        sent,
        got,
        base,
        inverse,
        toward_low,
        toward_high,
        margin_low,
        margin_high,
        ends_out,
        ends_in,
        back,
        norm_out,
        norm_x,
        norm_mid,
        src_sem,
        const_sem,
        small_sem,
        go_send,
        go_recv,
        ends_send,
        ends_recv,
        back_send,
        back_recv,
        norm_send,
        norm_recv,
    ) = refs[19:]
    depth_in, rows_in, rows_out, planes_in, planes_out, mu_planes, mu_rows, _ = consts

    blk = lax.axis_index("blk")
    py = lax.axis_index("py")
    pz = lax.axis_index("pz")
    place = py * PZ + pz

    def wrapped(a, n):
        return jnp.where(a >= n, a - n, a)

    def peer(step):
        to_py = wrapped(py + step % PY, PY)
        to_pz = wrapped(pz + step // PY, PZ)
        return to_py, to_pz, to_py * PZ + to_pz

    def everyone(visit):
        def one(near, to_pz):
            to_py = wrapped(py + near, PY)
            visit(to_py, to_pz, to_py * PZ + to_pz)

        def column(far, carry):
            to_pz = wrapped(pz + far, PZ)
            for near in range(PY):
                one(near, to_pz)
            return carry

        for near in range(1, PY):
            one(near, pz)
        lax.fori_loop(1, PZ, column, 0)

    barrier = pltpu.get_barrier_semaphore()

    def greet(to_py, to_pz, to):
        pl.semaphore_signal(barrier, inc=1, device_id=(blk, to_py, to_pz), device_id_type=MESH)

    loads = [pltpu.make_async_copy(source.at[y], src.at[y], src_sem.at[y]) for y in range(ROWS)]
    fetches = [pltpu.make_async_copy(a, b, const_sem.at[i]) for i, (a, b) in enumerate(zip(consts_hbm, consts))]
    smalls = [
        pltpu.make_async_copy(a, b, small_sem.at[i])
        for i, (a, b) in enumerate(
            (
                (conduct_hbm, conduct),
                (neighbours_hbm, neighbours),
                (orient_hbm, orient),
                (spectrum_hbm, depth_spectrum),
            )
        )
    ]
    fetches[0].start()
    for load in loads:
        load.start()
    everyone(greet)
    for step in range(1, BLOCKS):
        pl.semaphore_signal(
            barrier, inc=1, device_id=(wrapped(blk + step, BLOCKS), py, pz), device_id_type=MESH
        )
    for small in smalls:
        small.start()
    for fetch in fetches[1:]:
        fetch.start()

    fetches[0].wait()
    squares = jnp.zeros((8, 128), F32)
    for y in range(ROWS):
        loads[y].wait()
        cells = src[y]
        squares = squares + jnp.sum((cells * cells).reshape(BX // 8, 8, NZ), axis=0)
        hi, lo = split(cells)
        z = dot(depth_in[...], jnp.concatenate([hi, lo, hi], axis=1), NT)
        for h in range(HALVES):
            for x in range(2):
                sent[h, pl.ds(4 * x + y, PLANE, stride=8), :] = z[
                    PLANE * h : PLANE * (h + 1), 128 * x : 128 * (x + 1)
                ]
    own_squares = jnp.sum(jnp.sum(squares, axis=0, keepdims=True), axis=1, keepdims=True)

    pl.semaphore_wait(barrier, PLANE - 1 + BLOCKS - 1)

    def tile(d):
        return pl.ds(pl.multiple_of(d * 8, 8), 8)

    def exchange(src_ref, dst_ref, send_sem, recv_sem, h):
        def send(to_py, to_pz, to):
            pltpu.make_async_remote_copy(
                src_ref=src_ref.at[h, tile(to), :],
                dst_ref=dst_ref.at[h, tile(place), :],
                send_sem=send_sem.at[h],
                recv_sem=recv_sem.at[h],
                device_id=(blk, to_py, to_pz),
                device_id_type=MESH,
            ).start()

        everyone(send)
        dst_ref[h, tile(place), :] = src_ref[h, tile(place), :]

    def all_of(src_ref, dst_ref, send_sem, recv_sem, h):
        others = pl.ds(0, (PLANE - 1) * 8)
        return pltpu.make_async_remote_copy(
            src_ref=src_ref.at[h, others, :],
            dst_ref=dst_ref.at[h, others, :],
            send_sem=send_sem.at[h],
            recv_sem=recv_sem.at[h],
            device_id=(blk, wrapped(py + 1, PY), pz),
            device_id_type=MESH,
        )

    for h in range(HALVES):
        exchange(sent, got, go_send, go_recv, h)

    for wait in smalls + fetches[1:]:
        wait.wait()

    c0 = conduct[0]
    c1 = conduct[1]
    c2 = conduct[2]

    order = [jnp.int32(0)]
    for b in range(BLOCKS):
        order[0] = order[0] + b * (neighbours[0, b] == -1).astype(jnp.int32)
    for m in range(1, BLOCKS):
        following = jnp.int32(0)
        for b in range(BLOCKS):
            following = following + neighbours[1, b] * (order[m - 1] == b).astype(jnp.int32)
        order.append(following)
    is_at = [[(order[m] == b).astype(F32) for b in range(BLOCKS)] for m in range(BLOCKS)]
    own_at = [(order[m] == blk).astype(F32) for m in range(BLOCKS)]
    block_flips = [(orient[b] == 1).astype(F32) for b in range(BLOCKS)]
    flips = [sum(is_at[m][b] * block_flips[b] for b in range(BLOCKS)) for m in range(BLOCKS)]
    own_flip = sum(own_at[m] * flips[m] for m in range(BLOCKS))

    row_id = lax.broadcasted_iota(jnp.int32, (8, MODES), 0)

    def pick(flag, yes, no):
        return yes * flag + no * (1.0 - flag)

    plane_id = lax.broadcasted_iota(jnp.int32, (BX, MODES), 0).astype(F32)
    margin_id = lax.broadcasted_iota(jnp.int32, (OV, MODES), 0).astype(F32)
    greens = []
    for h in range(HALVES):
        shift = c1 * mu_rows[...] + c2 * depth_spectrum[PLANE * h + place]
        inverse[h] = 1.0 / (c0 * jnp.concatenate([mu_planes[...]] * 2, axis=1) + shift)
        half = jnp.sqrt(shift / (4.0 * c0))
        square = half * half
        theta = 2.0 * jnp.log1p(half + square / (1.0 + jnp.sqrt(1.0 + square)))

        def power(n):
            return jnp.exp(-n * theta)

        def fall(n):
            return 1.0 - power(2.0 * n)

        scale = 1.0 / (fall(1.0) * fall(385.0))
        f64, f65, f320, f321 = fall(64.0), fall(65.0), fall(320.0), fall(321.0)
        table = {
            (0, 0): power(1.0) * f64 * f321 * scale,
            (0, 1): power(2.0) * f64 * f320 * scale,
            (0, 2): power(257.0) * f64 * f65 * scale,
            (0, 3): power(258.0) * f64 * f64 * scale,
            (1, 1): power(1.0) * f65 * f320 * scale,
            (1, 2): power(256.0) * f65 * f65 * scale,
        }
        for a, b, c, d in ((1, 3, 0, 2), (2, 2, 1, 1), (2, 3, 0, 1), (3, 3, 0, 0)):
            table[a, b] = table[c, d]
        for a in range(4):
            for b in range(a):
                table[a, b] = table[b, a]
        greens.append((table, jnp.exp(theta) * f65 / f64))
        rise = jnp.exp(-plane_id * theta)
        drop = jnp.exp((plane_id - float(BX)) * theta)
        edge = f64 * scale
        far_low = drop * power(64.0)
        far_high = rise * power(65.0)
        toward_low[h] = rise * (power(2.0) * edge) * (1.0 - far_low * far_low)
        toward_high[h] = drop * (power(1.0) * edge) * (1.0 - far_high * far_high)
        inside = jnp.exp((margin_id - float(OV)) * theta)
        margin_low[h] = jnp.exp(-margin_id * theta) * ((1.0 - inside * inside) / f64)
        outside = jnp.exp(-(margin_id + 1.0) * theta)
        margin_high[h] = jnp.exp((margin_id - float(OV - 1)) * theta) * ((1.0 - outside * outside) / f64)

    def to_ends(h, step):
        return pltpu.make_async_remote_copy(
            src_ref=ends_out.at[h],
            dst_ref=ends_in.at[h, blk],
            send_sem=ends_send.at[h, step - 1],
            recv_sem=ends_recv.at[h, step - 1],
            device_id=(wrapped(blk + step, BLOCKS), py, pz),
            device_id_type=MESH,
        )

    def summed(x):
        return jnp.sum(x, axis=0, keepdims=True)

    lane = lax.broadcasted_iota(jnp.int32, (1, 128), 1)

    def total(x):
        return jnp.sum(x, axis=1, keepdims=True)

    def norm_copy(src_ref, dst_ref, stage, step):
        device = (blk, py, wrapped(pz + step, PZ)) if stage == 0 else (blk, wrapped(py + step, PY), pz)
        return pltpu.make_async_remote_copy(
            src_ref=src_ref,
            dst_ref=dst_ref.at[pz if stage == 0 else py],
            send_sem=norm_send.at[stage, step - 1],
            recv_sem=norm_recv.at[stage, step - 1],
            device_id=device,
            device_id_type=MESH,
        )

    change_1 = jnp.zeros((1, MODES), F32)
    change_2 = jnp.zeros((1, MODES), F32)
    total_squares = jnp.zeros((1, 1), F32)
    zero = jnp.zeros((1, MODES), F32)
    for h in range(HALVES):
        table, ratio = greens[h]
        all_of(sent, got, go_send, go_recv, h).wait_recv()
        plane = jnp.concatenate([assembled(got, h, r) for r in range(ROWS)], axis=0)
        held = times_right(plane.T, (rows_in[0], rows_in[1]), NN)
        near = (
            jnp.where(row_id == 0, summed(held * toward_low[h]) * (1.0 / c0), 0.0)
            + jnp.where(row_id == 1, summed(held * toward_high[h]) * (1.0 / c0), 0.0)
            + jnp.where(row_id == 2, summed(held[:OV] * margin_low[h]) * (1.0 / c0), 0.0)
            + jnp.where(row_id == 3, summed(held[BX - OV :] * margin_high[h]) * (1.0 / c0), 0.0)
            + jnp.where(row_id == 4, own_squares, 0.0)
        )
        ends_out[h] = near
        ends_in[h, blk] = near
        for step in range(1, BLOCKS):
            to_ends(h, step).start()

        solved_modes = times((planes_in[0], planes_in[1]), held, NN) * inverse[h]
        base[h] = times((planes_out[0], planes_out[1]), solved_modes, NN)

        for step in range(1, BLOCKS):
            to_ends(h, step).wait_recv()
        tiles = [ends_in[h, b] for b in range(BLOCKS)]
        if h == 0:
            for b in range(BLOCKS):
                total_squares = total_squares + tiles[b][4:5, :1]
        first, low, high = [], [], []
        for m in range(BLOCKS):
            at = sum(tiles[b] * is_at[m][b] for b in range(BLOCKS))
            left = pick(flips[m], at[1:2], at[0:1])
            right = pick(flips[m], at[0:1], at[1:2])
            first.append([left, left * ratio, right * ratio, right])
            low.append(pick(flips[m], at[3:4], at[2:3]))
            high.append(pick(flips[m], at[2:3], at[3:4]))
        outer = [
            [high[m - 1] if m > 0 else zero, zero, zero, low[m + 1] if m < BLOCKS - 1 else zero]
            for m in range(BLOCKS)
        ]

        def solved(m, p, sources):
            return first[m][p] + sum(table[p, q] * sources[m][q] for q in range(4))

        def jumps(sources):
            last = BLOCKS - 1
            left = [solved(m + 1, 1, sources) - solved(m, 3, sources) for m in range(last)]
            left.append(-solved(last, 3, sources))
            right = [solved(m, 2, sources) - solved(m + 1, 0, sources) for m in range(last)]
            right.append(-solved(0, 0, sources))
            return left, right

        def with_jumps(left, right):
            result = [list(o) for o in outer]
            for m in range(BLOCKS - 1):
                result[m][2] = left[m]
                result[m][3] = outer[m][3] + right[m]
                result[m + 1][1] = right[m]
                result[m + 1][0] = outer[m + 1][0] + left[m]
            result[BLOCKS - 1][2] = left[BLOCKS - 1]
            result[0][1] = right[BLOCKS - 1]
            return result

        left_1, right_1 = jumps(outer)
        left_2, right_2 = jumps(with_jumps(left_1, right_1))
        for a, b in zip(left_1 + right_1, left_2 + right_2):
            change_1 = change_1 + a * a
            change_2 = change_2 + (b - a) * (b - a)
        final = with_jumps(left_2, right_2)
        at_low = sum(own_at[m] * (final[m][0] + ratio * final[m][1]) for m in range(BLOCKS))
        at_high = sum(own_at[m] * (final[m][3] + ratio * final[m][2]) for m in range(BLOCKS))
        at_low, at_high = pick(own_flip, at_high, at_low), pick(own_flip, at_low, at_high)

        if h == HALVES - 1:
            partial = (
                jnp.where(lane == 0, total_squares, 0.0)
                + jnp.where(lane == 1, total(change_1) * (c0 * c0), 0.0)
                + jnp.where(lane == 2, total(change_2) * (c0 * c0), 0.0)
            )
            norm_out[...] = partial
            norm_x[pz] = partial
            for step in range(1, PZ):
                norm_copy(norm_out, norm_x, 0, step).start()

        across = base[h] + toward_low[h] * at_low + toward_high[h] * at_high
        plane = times((rows_out[0], rows_out[1]), across, NT)
        for r in range(ROWS):
            for x in range(2):
                back[h, pl.ds(4 * x + r, PLANE, stride=8), :] = plane[
                    PLANE * r : PLANE * (r + 1), 128 * x : 128 * (x + 1)
                ]
        exchange(back, returned, back_send, back_recv, h)

    for step in range(1, PZ):
        norm_copy(norm_out, norm_x, 0, step).wait_recv()
    partial = sum(norm_x[i] for i in range(PZ))
    norm_mid[...] = partial
    norm_z[py] = partial
    for step in range(1, PY):
        norm_copy(norm_mid, norm_z, 1, step).start()

    all_of(back, returned, back_send, back_recv, 0).wait_recv()
    for r in range(ROWS):
        partial_out[r] = depth_back(returned, 0, r, depth_out)

    for h in range(HALVES):
        all_of(sent, got, go_send, go_recv, h).wait_send()
        for step in range(1, BLOCKS):
            to_ends(h, step).wait_send()
    for step in range(1, PZ):
        norm_copy(norm_out, norm_x, 0, step).wait_send()
    all_of(back, returned, back_send, back_recv, 0).wait_send()
    all_of(back, returned, back_send, back_recv, 1).wait_recv()
    for step in range(1, PY):
        norm_copy(norm_mid, norm_z, 1, step).wait_recv()
    all_of(back, returned, back_send, back_recv, 1).wait_send()
    for step in range(1, PY):
        norm_copy(norm_mid, norm_z, 1, step).wait_send()


def finish(returned, partial_out, norm_z, depth_out, out, norms, result, out_sem):
    copies = []
    for r in range(ROWS):
        result[r] = partial_out[r] + depth_back(returned, 1, r, depth_out)
        copies.append(pltpu.make_async_copy(result.at[r], out.at[r], out_sem.at[r]))
        copies[r].start()
    lane = lax.broadcasted_iota(jnp.int32, (1, 128), 1)
    root = jnp.sqrt(sum(norm_z[i] for i in range(PY)) / CELLS)
    for i in range(3):
        norms[i] = jnp.sum(jnp.where(lane == i, root, 0.0))
    for copy in copies:
        copy.wait()


def shards(source, conduct, neighbours, orient):
    consts = tables()
    any_space = pl.BlockSpec(memory_space=pltpu.HBM)
    smem = pl.BlockSpec(memory_space=pltpu.SMEM)
    vmem = pl.BlockSpec(memory_space=pltpu.VMEM)
    dma = pltpu.SemaphoreType.DMA
    chunked = (HALVES, PLANE * 8, 128)
    cells = pltpu.VMEM((ROWS, BX, NZ), F32)
    limit = 24 * 1024 * 1024
    handed = pl.pallas_call(
        kernel,
        name="schwarz",
        out_shape=(
            jax.ShapeDtypeStruct(chunked, F32),
            jax.ShapeDtypeStruct((ROWS, BX, NZ), F32),
            jax.ShapeDtypeStruct((PY, 1, 128), F32),
            jax.ShapeDtypeStruct(consts[-1].shape, BF16),
        ),
        in_specs=[any_space] * (5 + len(consts)),
        out_specs=(vmem,) * 4,
        scratch_shapes=[pltpu.VMEM(c.shape, c.dtype) for c in consts[:-1]]
        + [
            pltpu.SMEM((3,), F32),
            pltpu.SMEM((2, BLOCKS), jnp.int32),
            pltpu.SMEM((BLOCKS,), jnp.int32),
            pltpu.SMEM((NZ,), F32),
            cells,
            pltpu.VMEM(chunked, F32),
            pltpu.VMEM(chunked, F32),
            pltpu.VMEM((HALVES, BX, MODES), F32),
            pltpu.VMEM((HALVES, EXT, MODES), F32),
            pltpu.VMEM((HALVES, BX, MODES), F32),
            pltpu.VMEM((HALVES, BX, MODES), F32),
            pltpu.VMEM((HALVES, OV, MODES), F32),
            pltpu.VMEM((HALVES, OV, MODES), F32),
            pltpu.VMEM((HALVES, 8, MODES), F32),
            pltpu.VMEM((HALVES, BLOCKS, 8, MODES), F32),
            pltpu.VMEM(chunked, F32),
            pltpu.VMEM((1, 128), F32),
            pltpu.VMEM((PZ, 1, 128), F32),
            pltpu.VMEM((1, 128), F32),
            dma((ROWS,)),
            dma((len(consts),)),
            dma((4,)),
            dma((HALVES,)),
            dma((HALVES,)),
            dma((HALVES, BLOCKS - 1)),
            dma((HALVES, BLOCKS - 1)),
            dma((HALVES,)),
            dma((HALVES,)),
            dma((2, PZ - 1)),
            dma((2, PZ - 1)),
        ],
        compiler_params=pltpu.CompilerParams(collective_id=0, has_side_effects=True, vmem_limit_bytes=limit),
    )(
        *[
            pltpu.with_memory_space_constraint(jnp.asarray(a), pltpu.HBM)
            for a in (
                source,
                conduct,
                neighbours.T,
                orient,
                eigenvalues(NZ).astype(np.float32),
                *consts,
            )
        ]
    )
    return pl.pallas_call(
        finish,
        name="finish",
        out_shape=(
            jax.ShapeDtypeStruct((ROWS, BX, NZ), F32),
            jax.ShapeDtypeStruct((3,), F32),
        ),
        in_specs=[vmem] * 4,
        out_specs=(any_space, smem),
        scratch_shapes=[cells, dma((ROWS,))],
        compiler_params=pltpu.CompilerParams(vmem_limit_bytes=limit),
    )(*handed)


def solution(mesh):
    cells = P(("py", "pz"), "blk", None)
    return jax.shard_map(
        shards, mesh=mesh, in_specs=(cells, P(), P(), P()), out_specs=(cells, P()), check_vma=False
    )
```

```python
import functools

import jax
import jax.numpy as jnp
import ml_dtypes
import numpy as np
from jax import lax
from jax.experimental import pallas as pl
from jax.experimental.pallas import tpu as pltpu
from jax.sharding import PartitionSpec as P

NY = 256
NZ = 128
BX = 256
OV = 64
EXT = 384
BLOCKS = 4
PY = 8
PZ = 8
PLANE = PY * PZ
ROWS = NY // PLANE
HALVES = 2
MODES = 256
MESH = pl.DeviceIdType.MESH
F32 = jnp.float32
BF16 = jnp.bfloat16
NN = (((1,), (0,)), ((), ()))
NT = (((1,), (1,)), ((), ()))
CELLS = float(BLOCKS * BX * NY * NZ)
TN = (((0,), (0,)), ((), ()))
SLOTS = 5
CONSTS = 13
EARLY = 3


def basis(n):
    j = np.arange(1, n + 1)
    m = (j[:, None] * j[None, :]) % (2 * (n + 1))
    return np.sqrt(2.0 / (n + 1)) * np.sin(np.pi * m / (n + 1))


def eigenvalues(n):
    return 4.0 * np.sin(np.pi * np.arange(1, n + 1) / (2.0 * (n + 1))) ** 2


def halves(a):
    a = a.astype(np.float32)
    hi = a.astype(ml_dtypes.bfloat16)
    lo = (a - hi.astype(np.float32)).astype(ml_dtypes.bfloat16)
    return np.stack([hi, lo])


@functools.lru_cache(None)
def tables():
    depth = halves(basis(NZ))
    rows = basis(NY)
    planes = basis(EXT)
    first = ROWS * np.arange(PLANE)
    outer_rows = rows[np.concatenate([first, first + ROWS - 1])]
    inner_rows = np.concatenate([rows[first + 1], rows[first + 2]], axis=1)
    inner = np.zeros((BX, BX))
    inner[1:-1, :-2] = basis(BX - 2)
    mu_inner = np.concatenate([eigenvalues(BX - 2), np.ones(2)])[None, :]
    rims = np.zeros((128, 2 * BX))
    rims[:4] = np.concatenate(
        [np.stack([inner[1], inner[-2]] * 2), np.stack([inner[1], inner[-2], -inner[1], -inner[-2]])], axis=1
    )
    planes_in = planes[OV : OV + BX].T
    depth_in = np.concatenate([depth[0], depth[0], depth[1]], axis=1)
    depth_out = np.stack(
        [
            np.concatenate([part[PLANE * h : PLANE * (h + 1)] for part in (depth[0], depth[0], depth[1])], axis=0)
            for h in range(HALVES)
        ]
    )
    return (
        depth_in,
        mu_inner.astype(np.float32),
        (eigenvalues(NZ)[:, None] * np.ones((1, 128))).astype(np.float32),
        halves(outer_rows),
        halves(inner_rows),
        halves(planes_in),
        halves(planes_in.T),
        (eigenvalues(EXT)[:, None] * np.ones((1, 128))).astype(np.float32),
        eigenvalues(NY)[None, :].astype(np.float32),
        halves(inner),
        halves(inner.T),
        halves(rims),
        depth_out,
    )


def split(x):
    hi = x.astype(BF16)
    return hi, (x - hi.astype(F32)).astype(BF16)


def dot(a, b, dims):
    return lax.dot_general(a, b, dimension_numbers=dims, preferred_element_type=F32)


def times(table, x, dims):
    hi, lo = split(x)
    return dot(table[0], hi, dims) + (dot(table[0], lo, dims) + dot(table[1], hi, dims))


def times_right(x, table, dims):
    hi, lo = split(x)
    return dot(hi, table[0], dims) + (dot(lo, table[0], dims) + dot(hi, table[1], dims))


def row_of(ref, h, slot):
    return ref[h, pl.ds(slot, PLANE, stride=SLOTS), :]


def outer_row(ref, h, r):
    return jnp.concatenate([row_of(ref, h, 2 * r + x) for x in range(2)], axis=1)


def restored(returned, h, local, by_row, by_plane, inner, inner_back, rims, depth_out):
    low_row = outer_row(returned, h, 0)
    high_row = outer_row(returned, h, 1)
    rim = row_of(returned, h, 4)
    from_rows = times_right(
        jnp.concatenate([low_row + high_row, low_row - high_row], axis=0), (inner[0], inner[1]), NN
    )
    from_rim = times_right(rim, (rims[0], rims[1]), NN)
    from_rim = jnp.concatenate([from_rim[:, :BX], from_rim[:, BX:]], axis=0)
    both = times_right(
        local[h] + by_row[h] * from_rows + by_plane[h] * from_rim, (inner_back[0], inner_back[1]), NN
    )
    plane = lax.broadcasted_iota(jnp.int32, (PLANE, BX), 1)

    def edged(cells, slot):
        cells = jnp.where(plane == 0, rim[:, slot : slot + 1], cells)
        return jnp.where(plane == BX - 1, rim[:, slot + 1 : slot + 2], cells)

    even, odd = both[:PLANE], both[PLANE:]
    rows = (low_row, edged(even + odd, 0), edged(even - odd, 2), high_row)
    return [depth_back(cells, depth_out[h]) for cells in rows]


def depth_back(cells, table):
    hi, lo = split(cells)
    return dot(jnp.concatenate([hi, lo, hi], axis=0), table, TN)


def kernel(source, conduct_hbm, neighbours_hbm, orient_hbm, spectrum_hbm, *refs):
    consts_hbm = refs[:CONSTS]
    returned, partial_out, norm_z, local, by_row, by_plane, inner, inner_back, rims, depth_out = refs[
        CONSTS : CONSTS + 10
    ]
    consts = refs[CONSTS + 10 : 2 * CONSTS + 6] + (inner, inner_back, rims, depth_out)
    (
        conduct,
        neighbours,
        orient,
        depth_spectrum,
        src,
        sent,
        got,
        base,
        inverse,
        toward_low,
        toward_high,
        margin_low,
        margin_high,
        ends_out,
        ends_in,
        back,
        norm_out,
        norm_x,
        norm_mid,
        src_sem,
        const_sem,
        small_sem,
        go_send,
        go_recv,
        ends_send,
        ends_recv,
        back_send,
        back_recv,
        norm_send,
        norm_recv,
    ) = refs[2 * CONSTS + 6 :]
    depth_in, mu_inner, mu_depth, outer_rows, inner_rows, planes_in, planes_out, mu_planes, mu_rows = consts[:9]

    blk = lax.axis_index("blk")
    py = lax.axis_index("py")
    pz = lax.axis_index("pz")
    place = py * PZ + pz

    def wrapped(a, n):
        return jnp.where(a >= n, a - n, a)

    def peer(step):
        to_py = wrapped(py + step % PY, PY)
        to_pz = wrapped(pz + step // PY, PZ)
        return to_py, to_pz, to_py * PZ + to_pz

    def everyone(visit):
        def one(near, to_pz):
            to_py = wrapped(py + near, PY)
            visit(to_py, to_pz, to_py * PZ + to_pz)

        def column(far, carry):
            to_pz = wrapped(pz + far, PZ)
            for near in range(PY):
                one(near, to_pz)
            return carry

        for near in range(1, PY):
            one(near, pz)
        lax.fori_loop(1, PZ, column, 0)

    barrier = pltpu.get_barrier_semaphore()

    def greet(to_py, to_pz, to):
        pl.semaphore_signal(barrier, inc=1, device_id=(blk, to_py, to_pz), device_id_type=MESH)

    loads = [pltpu.make_async_copy(source.at[y], src.at[y], src_sem.at[y]) for y in range(ROWS)]
    fetches = [pltpu.make_async_copy(a, b, const_sem.at[i]) for i, (a, b) in enumerate(zip(consts_hbm, consts))]
    smalls = [
        pltpu.make_async_copy(a, b, small_sem.at[i])
        for i, (a, b) in enumerate(
            (
                (conduct_hbm, conduct),
                (neighbours_hbm, neighbours),
                (orient_hbm, orient),
                (spectrum_hbm, depth_spectrum),
            )
        )
    ]
    early = fetches[:EARLY] + fetches[9:11]
    late = fetches[EARLY:9] + fetches[11:]
    for start in smalls + loads + early:
        start.start()
    everyone(greet)
    for step in range(1, BLOCKS):
        pl.semaphore_signal(
            barrier, inc=1, device_id=(wrapped(blk + step, BLOCKS), py, pz), device_id_type=MESH
        )
    for fetch in late:
        fetch.start()

    fetches[0].wait()
    squares = jnp.zeros((8, 128), F32)
    rows = []
    for y in range(ROWS):
        loads[y].wait()
        cells = src[y]
        squares = squares + jnp.sum((cells * cells).reshape(BX // 8, 8, NZ), axis=0)
        hi, lo = split(cells)
        rows.append(dot(depth_in[...], jnp.concatenate([hi, lo, hi], axis=1), NT))
    own_squares = jnp.sum(jnp.sum(squares, axis=0, keepdims=True), axis=1, keepdims=True)

    for wait in smalls + early[1:]:
        wait.wait()
    c0 = conduct[0]
    c1 = conduct[1]
    c2 = conduct[2]

    base_part = c0 * mu_inner[...] + c2 * jnp.concatenate([mu_depth[...]] * 2, axis=1)
    weights = jnp.concatenate([0.5 / (base_part + c1), 0.5 / (base_part + 3.0 * c1)], axis=0)
    mixed = jnp.concatenate([rows[1] + rows[2], rows[1] - rows[2]], axis=0)
    inner_modes = times_right(mixed, (inner[0], inner[1]), NN) * weights
    for h in range(HALVES):
        own = [slice(NZ * q + PLANE * h, NZ * q + PLANE * (h + 1)) for q in range(2)]
        weight = jnp.concatenate([weights[part] for part in own], axis=0)
        local[h] = jnp.concatenate([inner_modes[part] for part in own], axis=0)
        by_row[h] = weight * c1
        by_plane[h] = weight * c0
    both = times_right(inner_modes, (inner_back[0], inner_back[1]), NN)
    solved_rows = (both[:NZ] + both[NZ:], both[:NZ] - both[NZ:])
    lanes = lax.broadcasted_iota(jnp.int32, (NZ, 128), 1)
    rim = jnp.zeros((NZ, 128), F32)
    for r in range(2):
        near, far = solved_rows[r][:, :128], solved_rows[r][:, 128:]
        at_first = rows[1 + r][:, :128] + c0 * pltpu.roll(near, 127, 1)
        at_last = rows[1 + r][:, 128:] + c0 * pltpu.roll(far, 1, 1)
        part = jnp.where(lanes == 0, at_first, 0.0)
        part = jnp.where(lanes == 127, at_last, part)
        part = jnp.where(lanes == OV, near, part)
        part = jnp.where(lanes == OV - 1, far, part)
        rim = rim + (part if r == 0 else pltpu.roll(part, 2, 1))
    outer_cells = (rows[0] + c1 * solved_rows[0], rows[3] + c1 * solved_rows[1])
    for h in range(HALVES):
        part = slice(PLANE * h, PLANE * (h + 1))
        for r in range(2):
            for x in range(2):
                sent[h, pl.ds(2 * r + x, PLANE, stride=SLOTS), :] = outer_cells[r][
                    part, 128 * x : 128 * (x + 1)
                ]
        sent[h, pl.ds(4, PLANE, stride=SLOTS), :] = rim[part]

    pl.semaphore_wait(barrier, PLANE - 1 + BLOCKS - 1)

    def tile(d):
        return pl.ds(d * SLOTS, SLOTS)

    def exchange(src_ref, dst_ref, send_sem, recv_sem, h):
        def send(to_py, to_pz, to):
            pltpu.make_async_remote_copy(
                src_ref=src_ref.at[h, tile(to), :],
                dst_ref=dst_ref.at[h, tile(place), :],
                send_sem=send_sem.at[h],
                recv_sem=recv_sem.at[h],
                device_id=(blk, to_py, to_pz),
                device_id_type=MESH,
            ).start()

        everyone(send)
        dst_ref[h, tile(place), :] = src_ref[h, tile(place), :]

    def all_of(src_ref, dst_ref, send_sem, recv_sem, h):
        others = pl.ds(0, (PLANE - 1) * SLOTS)
        return pltpu.make_async_remote_copy(
            src_ref=src_ref.at[h, others, :],
            dst_ref=dst_ref.at[h, others, :],
            send_sem=send_sem.at[h],
            recv_sem=recv_sem.at[h],
            device_id=(blk, wrapped(py + 1, PY), pz),
            device_id_type=MESH,
        )

    for h in range(HALVES):
        exchange(sent, got, go_send, go_recv, h)

    for fetch in late:
        fetch.wait()

    order = [jnp.int32(0)]
    for b in range(BLOCKS):
        order[0] = order[0] + b * (neighbours[0, b] == -1).astype(jnp.int32)
    for m in range(1, BLOCKS):
        following = jnp.int32(0)
        for b in range(BLOCKS):
            following = following + neighbours[1, b] * (order[m - 1] == b).astype(jnp.int32)
        order.append(following)
    is_at = [[(order[m] == b).astype(F32) for b in range(BLOCKS)] for m in range(BLOCKS)]
    own_at = [(order[m] == blk).astype(F32) for m in range(BLOCKS)]
    block_flips = [(orient[b] == 1).astype(F32) for b in range(BLOCKS)]
    flips = [sum(is_at[m][b] * block_flips[b] for b in range(BLOCKS)) for m in range(BLOCKS)]
    own_flip = sum(own_at[m] * flips[m] for m in range(BLOCKS))

    row_id = lax.broadcasted_iota(jnp.int32, (8, MODES), 0)

    def pick(flag, yes, no):
        return yes * flag + no * (1.0 - flag)

    plane_id = lax.broadcasted_iota(jnp.int32, (BX, MODES), 0).astype(F32)
    margin_id = lax.broadcasted_iota(jnp.int32, (OV, MODES), 0).astype(F32)
    greens = []
    for h in range(HALVES):
        shift = c1 * mu_rows[...] + c2 * depth_spectrum[PLANE * h + place]
        inverse[h] = 1.0 / (c0 * jnp.concatenate([mu_planes[...]] * 2, axis=1) + shift)
        half = jnp.sqrt(shift / (4.0 * c0))
        square = half * half
        theta = 2.0 * jnp.log1p(half + square / (1.0 + jnp.sqrt(1.0 + square)))

        def power(n):
            return jnp.exp(-n * theta)

        def fall(n):
            return 1.0 - power(2.0 * n)

        scale = 1.0 / (fall(1.0) * fall(385.0))
        f64, f65, f320, f321 = fall(64.0), fall(65.0), fall(320.0), fall(321.0)
        table = {
            (0, 0): power(1.0) * f64 * f321 * scale,
            (0, 1): power(2.0) * f64 * f320 * scale,
            (0, 2): power(257.0) * f64 * f65 * scale,
            (0, 3): power(258.0) * f64 * f64 * scale,
            (1, 1): power(1.0) * f65 * f320 * scale,
            (1, 2): power(256.0) * f65 * f65 * scale,
        }
        for a, b, c, d in ((1, 3, 0, 2), (2, 2, 1, 1), (2, 3, 0, 1), (3, 3, 0, 0)):
            table[a, b] = table[c, d]
        for a in range(4):
            for b in range(a):
                table[a, b] = table[b, a]
        greens.append((table, jnp.exp(theta) * f65 / f64))
        rise = jnp.exp(-plane_id * theta)
        drop = jnp.exp((plane_id - float(BX)) * theta)
        edge = f64 * scale
        far_low = drop * power(64.0)
        far_high = rise * power(65.0)
        toward_low[h] = rise * (power(2.0) * edge) * (1.0 - far_low * far_low)
        toward_high[h] = drop * (power(1.0) * edge) * (1.0 - far_high * far_high)
        inside = jnp.exp((margin_id - float(OV)) * theta)
        margin_low[h] = jnp.exp(-margin_id * theta) * ((1.0 - inside * inside) / f64)
        outside = jnp.exp(-(margin_id + 1.0) * theta)
        margin_high[h] = jnp.exp((margin_id - float(OV - 1)) * theta) * ((1.0 - outside * outside) / f64)

    def to_ends(h, step):
        return pltpu.make_async_remote_copy(
            src_ref=ends_out.at[h],
            dst_ref=ends_in.at[h, blk],
            send_sem=ends_send.at[h, step - 1],
            recv_sem=ends_recv.at[h, step - 1],
            device_id=(wrapped(blk + step, BLOCKS), py, pz),
            device_id_type=MESH,
        )

    def summed(x):
        return jnp.sum(x, axis=0, keepdims=True)

    lane = lax.broadcasted_iota(jnp.int32, (1, 128), 1)

    def total(x):
        return jnp.sum(x, axis=1, keepdims=True)

    def norm_copy(src_ref, dst_ref, stage, step):
        device = (blk, py, wrapped(pz + step, PZ)) if stage == 0 else (blk, wrapped(py + step, PY), pz)
        return pltpu.make_async_remote_copy(
            src_ref=src_ref,
            dst_ref=dst_ref.at[pz if stage == 0 else py],
            send_sem=norm_send.at[stage, step - 1],
            recv_sem=norm_recv.at[stage, step - 1],
            device_id=device,
            device_id_type=MESH,
        )

    change_1 = jnp.zeros((1, MODES), F32)
    change_2 = jnp.zeros((1, MODES), F32)
    total_squares = jnp.zeros((1, 1), F32)
    zero = jnp.zeros((1, MODES), F32)
    for h in range(HALVES):
        table, ratio = greens[h]
        all_of(sent, got, go_send, go_recv, h).wait_recv()
        plane = jnp.concatenate([outer_row(got, h, r) for r in range(2)], axis=0)
        held = times_right(plane.T, (outer_rows[0], outer_rows[1]), NN)
        extra = times_right(row_of(got, h, 4).T, (inner_rows[0], inner_rows[1]), NN)
        one, two = extra[:, :MODES], extra[:, MODES:]
        at_first = one[0:1] + two[2:3]
        at_last = one[127:128] + two[1:2]
        cut_low = (one[OV : OV + 1] + two[OV + 2 : OV + 3]) * c0
        cut_high = (one[OV - 1 : OV] + two[OV + 1 : OV + 2]) * c0
        held = jnp.concatenate(
            [
                held[:8] + jnp.where(row_id == 0, at_first, 0.0),
                held[8:-8],
                held[-8:] + jnp.where(row_id == 7, at_last, 0.0),
            ],
            axis=0,
        )
        near = (
            jnp.where(row_id == 0, summed(held * toward_low[h]) * (1.0 / c0), 0.0)
            + jnp.where(row_id == 1, summed(held * toward_high[h]) * (1.0 / c0), 0.0)
            + jnp.where(row_id == 2, (summed(held[:OV] * margin_low[h]) - cut_low * margin_low[h, OV - 1 : OV, :]) * (1.0 / c0), 0.0)
            + jnp.where(row_id == 3, (summed(held[BX - OV :] * margin_high[h]) - cut_high * margin_high[h, 0:1, :]) * (1.0 / c0), 0.0)
            + jnp.where(row_id == 4, own_squares, 0.0)
        )
        ends_out[h] = near
        ends_in[h, blk] = near
        for step in range(1, BLOCKS):
            to_ends(h, step).start()

        solved_modes = times((planes_in[0], planes_in[1]), held, NN) * inverse[h]
        base[h] = times((planes_out[0], planes_out[1]), solved_modes, NN)

        for step in range(1, BLOCKS):
            to_ends(h, step).wait_recv()
        tiles = [ends_in[h, b] for b in range(BLOCKS)]
        if h == 0:
            for b in range(BLOCKS):
                total_squares = total_squares + tiles[b][4:5, :1]
        first, low, high = [], [], []
        for m in range(BLOCKS):
            at = sum(tiles[b] * is_at[m][b] for b in range(BLOCKS))
            left = pick(flips[m], at[1:2], at[0:1])
            right = pick(flips[m], at[0:1], at[1:2])
            first.append([left, left * ratio, right * ratio, right])
            low.append(pick(flips[m], at[3:4], at[2:3]))
            high.append(pick(flips[m], at[2:3], at[3:4]))
        outer = [
            [high[m - 1] if m > 0 else zero, zero, zero, low[m + 1] if m < BLOCKS - 1 else zero]
            for m in range(BLOCKS)
        ]

        def solved(m, p, sources):
            return first[m][p] + sum(table[p, q] * sources[m][q] for q in range(4))

        def jumps(sources):
            last = BLOCKS - 1
            left = [solved(m + 1, 1, sources) - solved(m, 3, sources) for m in range(last)]
            left.append(-solved(last, 3, sources))
            right = [solved(m, 2, sources) - solved(m + 1, 0, sources) for m in range(last)]
            right.append(-solved(0, 0, sources))
            return left, right

        def with_jumps(left, right):
            result = [list(o) for o in outer]
            for m in range(BLOCKS - 1):
                result[m][2] = left[m]
                result[m][3] = outer[m][3] + right[m]
                result[m + 1][1] = right[m]
                result[m + 1][0] = outer[m + 1][0] + left[m]
            result[BLOCKS - 1][2] = left[BLOCKS - 1]
            result[0][1] = right[BLOCKS - 1]
            return result

        left_1, right_1 = jumps(outer)
        left_2, right_2 = jumps(with_jumps(left_1, right_1))
        for a, b in zip(left_1 + right_1, left_2 + right_2):
            change_1 = change_1 + a * a
            change_2 = change_2 + (b - a) * (b - a)
        final = with_jumps(left_2, right_2)
        at_low = sum(own_at[m] * (final[m][0] + ratio * final[m][1]) for m in range(BLOCKS))
        at_high = sum(own_at[m] * (final[m][3] + ratio * final[m][2]) for m in range(BLOCKS))
        at_low, at_high = pick(own_flip, at_high, at_low), pick(own_flip, at_low, at_high)

        if h == HALVES - 1:
            partial = (
                jnp.where(lane == 0, total_squares, 0.0)
                + jnp.where(lane == 1, total(change_1) * (c0 * c0), 0.0)
                + jnp.where(lane == 2, total(change_2) * (c0 * c0), 0.0)
            )
            norm_out[...] = partial
            norm_x[pz] = partial
            for step in range(1, PZ):
                norm_copy(norm_out, norm_x, 0, step).start()

        across = base[h] + toward_low[h] * at_low + toward_high[h] * at_high
        plane = times((outer_rows[0], outer_rows[1]), across, NT)
        ends = [across[:1], across[-1:]]
        rim_modes = jnp.concatenate(
            [
                sum(jnp.where(row_id == 2 * r + e, ends[e], 0.0) for e in range(2))
                for r in range(2)
            ],
            axis=1,
        )
        rim_modes = jnp.concatenate([rim_modes, jnp.zeros((120, 2 * MODES), F32)], axis=0)
        for r in range(2):
            for x in range(2):
                back[h, pl.ds(2 * r + x, PLANE, stride=SLOTS), :] = plane[
                    PLANE * r : PLANE * (r + 1), 128 * x : 128 * (x + 1)
                ]
        back[h, pl.ds(4, PLANE, stride=SLOTS), :] = times((inner_rows[0], inner_rows[1]), rim_modes, NT)
        exchange(back, returned, back_send, back_recv, h)

    for step in range(1, PZ):
        norm_copy(norm_out, norm_x, 0, step).wait_recv()
    partial = sum(norm_x[i] for i in range(PZ))
    norm_mid[...] = partial
    norm_z[py] = partial
    for step in range(1, PY):
        norm_copy(norm_mid, norm_z, 1, step).start()

    all_of(back, returned, back_send, back_recv, 0).wait_recv()
    for r, cells in enumerate(
        restored(returned, 0, local, by_row, by_plane, inner, inner_back, rims, depth_out)
    ):
        partial_out[r] = cells

    for h in range(HALVES):
        all_of(sent, got, go_send, go_recv, h).wait_send()
        for step in range(1, BLOCKS):
            to_ends(h, step).wait_send()
    for step in range(1, PZ):
        norm_copy(norm_out, norm_x, 0, step).wait_send()
    all_of(back, returned, back_send, back_recv, 0).wait_send()
    all_of(back, returned, back_send, back_recv, 1).wait_recv()
    for step in range(1, PY):
        norm_copy(norm_mid, norm_z, 1, step).wait_recv()
    all_of(back, returned, back_send, back_recv, 1).wait_send()
    for step in range(1, PY):
        norm_copy(norm_mid, norm_z, 1, step).wait_send()


def finish(returned, partial_out, norm_z, *refs):
    held, (out, norms, result, out_sem) = refs[:-4], refs[-4:]
    copies = []
    for r, cells in enumerate(restored(returned, 1, *held)):
        result[r] = partial_out[r] + cells
        copies.append(pltpu.make_async_copy(result.at[r], out.at[r], out_sem.at[r]))
        copies[r].start()
    lane = lax.broadcasted_iota(jnp.int32, (1, 128), 1)
    root = jnp.sqrt(sum(norm_z[i] for i in range(PY)) / CELLS)
    for i in range(3):
        norms[i] = jnp.sum(jnp.where(lane == i, root, 0.0))
    for copy in copies:
        copy.wait()


def shards(source, conduct, neighbours, orient):
    consts = tables()
    any_space = pl.BlockSpec(memory_space=pltpu.HBM)
    smem = pl.BlockSpec(memory_space=pltpu.SMEM)
    vmem = pl.BlockSpec(memory_space=pltpu.VMEM)
    dma = pltpu.SemaphoreType.DMA
    chunked = (HALVES, PLANE * SLOTS, 128)
    modal = (HALVES, 2 * PLANE, BX)
    cells = pltpu.VMEM((ROWS, BX, NZ), F32)
    limit = 24 * 1024 * 1024
    handed = pl.pallas_call(
        kernel,
        name="schwarz",
        out_shape=(
            jax.ShapeDtypeStruct(chunked, F32),
            jax.ShapeDtypeStruct((ROWS, BX, NZ), F32),
            jax.ShapeDtypeStruct((PY, 1, 128), F32),
            jax.ShapeDtypeStruct(modal, F32),
            jax.ShapeDtypeStruct(modal, F32),
            jax.ShapeDtypeStruct(modal, F32),
            *[jax.ShapeDtypeStruct(c.shape, BF16) for c in consts[-4:]],
        ),
        in_specs=[any_space] * (5 + len(consts)),
        out_specs=(vmem,) * 10,
        scratch_shapes=[pltpu.VMEM(c.shape, c.dtype) for c in consts[:-4]]
        + [
            pltpu.SMEM((3,), F32),
            pltpu.SMEM((2, BLOCKS), jnp.int32),
            pltpu.SMEM((BLOCKS,), jnp.int32),
            pltpu.SMEM((NZ,), F32),
            cells,
            pltpu.VMEM(chunked, F32),
            pltpu.VMEM(chunked, F32),
            pltpu.VMEM((HALVES, BX, MODES), F32),
            pltpu.VMEM((HALVES, EXT, MODES), F32),
            pltpu.VMEM((HALVES, BX, MODES), F32),
            pltpu.VMEM((HALVES, BX, MODES), F32),
            pltpu.VMEM((HALVES, OV, MODES), F32),
            pltpu.VMEM((HALVES, OV, MODES), F32),
            pltpu.VMEM((HALVES, 8, MODES), F32),
            pltpu.VMEM((HALVES, BLOCKS, 8, MODES), F32),
            pltpu.VMEM(chunked, F32),
            pltpu.VMEM((1, 128), F32),
            pltpu.VMEM((PZ, 1, 128), F32),
            pltpu.VMEM((1, 128), F32),
            dma((ROWS,)),
            dma((len(consts),)),
            dma((4,)),
            dma((HALVES,)),
            dma((HALVES,)),
            dma((HALVES, BLOCKS - 1)),
            dma((HALVES, BLOCKS - 1)),
            dma((HALVES,)),
            dma((HALVES,)),
            dma((2, PZ - 1)),
            dma((2, PZ - 1)),
        ],
        compiler_params=pltpu.CompilerParams(collective_id=0, has_side_effects=True, vmem_limit_bytes=limit),
    )(
        *[
            pltpu.with_memory_space_constraint(jnp.asarray(a), pltpu.HBM)
            for a in (
                source,
                conduct,
                neighbours.T,
                orient,
                eigenvalues(NZ).astype(np.float32),
                *consts,
            )
        ]
    )
    return pl.pallas_call(
        finish,
        name="finish",
        out_shape=(
            jax.ShapeDtypeStruct((ROWS, BX, NZ), F32),
            jax.ShapeDtypeStruct((3,), F32),
        ),
        in_specs=[vmem] * 10,
        out_specs=(any_space, smem),
        scratch_shapes=[cells, dma((ROWS,))],
        compiler_params=pltpu.CompilerParams(vmem_limit_bytes=limit),
    )(*handed)


def solution(mesh):
    cells = P(("py", "pz"), "blk", None)
    return jax.shard_map(
        shards, mesh=mesh, in_specs=(cells, P(), P(), P()), out_specs=(cells, P()), check_vma=False
    )
```

```python
import functools

import jax
import jax.numpy as jnp
import ml_dtypes
import numpy as np
from jax import lax
from jax.experimental import pallas as pl
from jax.experimental.pallas import tpu as pltpu
from jax.sharding import PartitionSpec as P

NY = 256
NZ = 128
BX = 256
OV = 64
EXT = 384
BLOCKS = 4
PY = 8
PZ = 8
PLANE = PY * PZ
ROWS = NY // PLANE
HALVES = 2
MODES = 256
MESH = pl.DeviceIdType.MESH
F32 = jnp.float32
BF16 = jnp.bfloat16
NN = (((1,), (0,)), ((), ()))
NT = (((1,), (1,)), ((), ()))
CELLS = float(BLOCKS * BX * NY * NZ)
TN = (((0,), (0,)), ((), ()))
BACK = 5
THERE = (5, 4)
CONSTS = 13
EARLY = 3


def basis(n):
    j = np.arange(1, n + 1)
    m = (j[:, None] * j[None, :]) % (2 * (n + 1))
    return np.sqrt(2.0 / (n + 1)) * np.sin(np.pi * m / (n + 1))


def eigenvalues(n):
    return 4.0 * np.sin(np.pi * np.arange(1, n + 1) / (2.0 * (n + 1))) ** 2


def halves(a):
    a = a.astype(np.float32)
    hi = a.astype(ml_dtypes.bfloat16)
    lo = (a - hi.astype(np.float32)).astype(ml_dtypes.bfloat16)
    return np.stack([hi, lo])


@functools.lru_cache(None)
def tables():
    depth = halves(basis(NZ))
    rows = basis(NY)
    planes = basis(EXT)
    first = ROWS * np.arange(PLANE)
    outer_rows = rows[np.concatenate([first, first + ROWS - 1])]
    inner_rows = np.concatenate([rows[first + 1], rows[first + 2]], axis=1)
    inner = np.zeros((BX, BX))
    inner[1:-1, :-2] = basis(BX - 2)
    mu_inner = np.concatenate([eigenvalues(BX - 2), np.ones(2)])[None, :]
    rims = np.zeros((128, 2 * BX))
    rims[:4] = np.concatenate(
        [np.stack([inner[1], inner[-2]] * 2), np.stack([inner[1], inner[-2], -inner[1], -inner[-2]])], axis=1
    )
    planes_in = planes[OV : OV + BX].T
    depth_in = np.concatenate([depth[0], depth[0], depth[1]], axis=1)
    depth_out = np.stack(
        [
            np.concatenate([part[PLANE * h : PLANE * (h + 1)] for part in (depth[0], depth[0], depth[1])], axis=0)
            for h in range(HALVES)
        ]
    )
    return (
        depth_in,
        mu_inner.astype(np.float32),
        (eigenvalues(NZ)[:, None] * np.ones((1, 128))).astype(np.float32),
        halves(outer_rows),
        halves(inner_rows),
        halves(planes_in),
        halves(planes_in.T),
        (eigenvalues(EXT)[:, None] * np.ones((1, 128))).astype(np.float32),
        eigenvalues(NY)[None, :].astype(np.float32),
        halves(inner),
        halves(inner.T),
        halves(rims),
        depth_out,
    )


def split(x):
    hi = x.astype(BF16)
    return hi, (x - hi.astype(F32)).astype(BF16)


def dot(a, b, dims):
    return lax.dot_general(a, b, dimension_numbers=dims, preferred_element_type=F32)


def times(table, x, dims):
    hi, lo = split(x)
    return dot(table[0], hi, dims) + (dot(table[0], lo, dims) + dot(table[1], hi, dims))


def times_right(x, table, dims):
    hi, lo = split(x)
    return dot(hi, table[0], dims) + (dot(lo, table[0], dims) + dot(hi, table[1], dims))


def row_of(ref, h, slot, slots):
    return ref[h, pl.ds(slot, PLANE, stride=slots), :]


def outer_row(ref, h, r, slots):
    return jnp.concatenate([row_of(ref, h, 2 * r + x, slots) for x in range(2)], axis=1)


def restored(returned, h, local, by_row, by_plane, inner, inner_back, rims, depth_out):
    low_row = outer_row(returned, h, 0, BACK)
    high_row = outer_row(returned, h, 1, BACK)
    yield 0, depth_back(low_row, depth_out[h])
    yield 3, depth_back(high_row, depth_out[h])
    rim = row_of(returned, h, 4, BACK)
    from_rows = times_right(
        jnp.concatenate([low_row + high_row, low_row - high_row], axis=0), (inner[0], inner[1]), NN
    )
    from_rim = times_right(rim, (rims[0], rims[1]), NN)
    from_rim = jnp.concatenate([from_rim[:, :BX], from_rim[:, BX:]], axis=0)
    both = times_right(
        local[h] + by_row[h] * from_rows + by_plane[h] * from_rim, (inner_back[0], inner_back[1]), NN
    )
    plane = lax.broadcasted_iota(jnp.int32, (PLANE, BX), 1)

    def edged(cells, slot):
        cells = jnp.where(plane == 0, rim[:, slot : slot + 1], cells)
        return jnp.where(plane == BX - 1, rim[:, slot + 1 : slot + 2], cells)

    even, odd = both[:PLANE], both[PLANE:]
    yield 1, depth_back(edged(even + odd, 0), depth_out[h])
    yield 2, depth_back(edged(even - odd, 2), depth_out[h])


def depth_back(cells, table):
    hi, lo = split(cells)
    return dot(jnp.concatenate([hi, lo, hi], axis=0), table, TN)


def kernel(source, conduct_hbm, neighbours_hbm, orient_hbm, spectrum_hbm, *refs):
    consts_hbm = refs[:CONSTS]
    returned, partial_out, norm_z, local, by_row, by_plane, inner, inner_back, rims, depth_out = refs[
        CONSTS : CONSTS + 10
    ]
    consts = refs[CONSTS + 10 : 2 * CONSTS + 6] + (inner, inner_back, rims, depth_out)
    (
        conduct,
        neighbours,
        orient,
        depth_spectrum,
        src,
        sent,
        got,
        held_modes,
        extras,
        base,
        inverse,
        toward_low,
        toward_high,
        margin_low,
        margin_high,
        ends_out,
        ends_in,
        back,
        norm_out,
        norm_x,
        norm_mid,
        src_sem,
        const_sem,
        small_sem,
        go_send,
        go_recv,
        ends_send,
        ends_recv,
        back_send,
        back_recv,
        norm_send,
        norm_recv,
    ) = refs[2 * CONSTS + 6 :]
    depth_in, mu_inner, mu_depth, outer_rows, inner_rows, planes_in, planes_out, mu_planes, mu_rows = consts[:9]

    blk = lax.axis_index("blk")
    py = lax.axis_index("py")
    pz = lax.axis_index("pz")
    place = py * PZ + pz

    def wrapped(a, n):
        return jnp.where(a >= n, a - n, a)

    def peer(step):
        to_py = wrapped(py + step % PY, PY)
        to_pz = wrapped(pz + step // PY, PZ)
        return to_py, to_pz, to_py * PZ + to_pz

    def everyone(visit):
        def one(near, to_pz):
            to_py = wrapped(py + near, PY)
            visit(to_py, to_pz, to_py * PZ + to_pz)

        def column(far, carry):
            to_pz = wrapped(pz + far, PZ)
            for near in (4, 3, 5, 2, 6, 1, 7, 0):
                one(near, to_pz)
            return carry

        lax.fori_loop(PZ // 2, PZ, column, 0)
        lax.fori_loop(1, PZ // 2, column, 0)
        for near in range(1, PY):
            one(near, pz)

    barrier = pltpu.get_barrier_semaphore()

    def greet(to_py, to_pz, to):
        pl.semaphore_signal(barrier, inc=1, device_id=(blk, to_py, to_pz), device_id_type=MESH)

    loads = [pltpu.make_async_copy(source.at[y], src.at[y], src_sem.at[y]) for y in range(ROWS)]
    fetches = [pltpu.make_async_copy(a, b, const_sem.at[i]) for i, (a, b) in enumerate(zip(consts_hbm, consts))]
    smalls = [
        pltpu.make_async_copy(a, b, small_sem.at[i])
        for i, (a, b) in enumerate(
            (
                (conduct_hbm, conduct),
                (neighbours_hbm, neighbours),
                (orient_hbm, orient),
                (spectrum_hbm, depth_spectrum),
            )
        )
    ]
    early = fetches[:EARLY] + fetches[9:11]
    late = fetches[EARLY:9] + fetches[11:]
    everyone(greet)
    for start in smalls + loads + early:
        start.start()
    for step in range(1, BLOCKS):
        pl.semaphore_signal(
            barrier, inc=1, device_id=(wrapped(blk + step, BLOCKS), py, pz), device_id_type=MESH
        )
    for fetch in late:
        fetch.start()

    fetches[0].wait()
    squares = jnp.zeros((8, 128), F32)
    rows = []
    for y in range(ROWS):
        loads[y].wait()
        cells = src[y]
        squares = squares + jnp.sum((cells * cells).reshape(BX // 8, 8, NZ), axis=0)
        hi, lo = split(cells)
        rows.append(dot(depth_in[...], jnp.concatenate([hi, lo, hi], axis=1), NT))
    own_squares = jnp.sum(jnp.sum(squares, axis=0, keepdims=True), axis=1, keepdims=True)

    for wait in smalls + early[1:]:
        wait.wait()
    c0 = conduct[0]
    c1 = conduct[1]
    c2 = conduct[2]

    base_part = c0 * mu_inner[...] + c2 * jnp.concatenate([mu_depth[...]] * 2, axis=1)
    weights = jnp.concatenate([0.5 / (base_part + c1), 0.5 / (base_part + 3.0 * c1)], axis=0)
    mixed = jnp.concatenate([rows[1] + rows[2], rows[1] - rows[2]], axis=0)
    inner_modes = times_right(mixed, (inner[0], inner[1]), NN) * weights
    for h in range(HALVES):
        own = [slice(NZ * q + PLANE * h, NZ * q + PLANE * (h + 1)) for q in range(2)]
        weight = jnp.concatenate([weights[part] for part in own], axis=0)
        local[h] = jnp.concatenate([inner_modes[part] for part in own], axis=0)
        by_row[h] = weight * c1
        by_plane[h] = weight * c0
    both = times_right(inner_modes, (inner_back[0], inner_back[1]), NN)
    solved_rows = (both[:NZ] + both[NZ:], both[:NZ] - both[NZ:])
    lanes = lax.broadcasted_iota(jnp.int32, (NZ, 128), 1)
    rim = jnp.zeros((NZ, 128), F32)
    for r in range(2):
        near, far = solved_rows[r][:, :128], solved_rows[r][:, 128:]
        at_first = rows[1 + r][:, :128] + c0 * pltpu.roll(near, 127, 1)
        at_last = rows[1 + r][:, 128:] + c0 * pltpu.roll(far, 1, 1)
        part = jnp.where(lanes == 0, at_first, 0.0)
        part = jnp.where(lanes == 127, at_last, part)
        part = jnp.where(lanes == OV, near, part)
        part = jnp.where(lanes == OV - 1, far, part)
        rim = rim + (part if r == 0 else pltpu.roll(part, 2, 1))
    outer_cells = (rows[0] + c1 * solved_rows[0], rows[3] + c1 * solved_rows[1])
    for h in range(HALVES):
        part = slice(PLANE * h, PLANE * (h + 1))
        for r in range(2):
            for x in range(2):
                sent[h, pl.ds(2 * r + x, PLANE, stride=THERE[h]), :] = outer_cells[r][
                    part, 128 * x : 128 * (x + 1)
                ]
    sent[0, pl.ds(4, PLANE, stride=THERE[0]), :] = rim[:PLANE] + pltpu.roll(rim[PLANE:], 4, 1)

    pl.semaphore_wait(barrier, PLANE - 1 + BLOCKS - 1)

    def exchange(src_ref, dst_ref, send_sem, recv_sem, h, slots):
        def tile(d):
            return pl.ds(d * slots, slots)

        def send(to_py, to_pz, to):
            pltpu.make_async_remote_copy(
                src_ref=src_ref.at[h, tile(to), :],
                dst_ref=dst_ref.at[h, tile(place), :],
                send_sem=send_sem.at[h],
                recv_sem=recv_sem.at[h],
                device_id=(blk, to_py, to_pz),
                device_id_type=MESH,
            ).start()

        everyone(send)
        dst_ref[h, tile(place), :] = src_ref[h, tile(place), :]

    def all_of(src_ref, dst_ref, send_sem, recv_sem, h, slots):
        others = pl.ds(0, (PLANE - 1) * slots)
        return pltpu.make_async_remote_copy(
            src_ref=src_ref.at[h, others, :],
            dst_ref=dst_ref.at[h, others, :],
            send_sem=send_sem.at[h],
            recv_sem=recv_sem.at[h],
            device_id=(blk, wrapped(py + 1, PY), pz),
            device_id_type=MESH,
        )

    for h in range(HALVES):
        exchange(sent, got, go_send, go_recv, h, THERE[h])

    for fetch in late:
        fetch.wait()

    order = [jnp.int32(0)]
    for b in range(BLOCKS):
        order[0] = order[0] + b * (neighbours[0, b] == -1).astype(jnp.int32)
    for m in range(1, BLOCKS):
        following = jnp.int32(0)
        for b in range(BLOCKS):
            following = following + neighbours[1, b] * (order[m - 1] == b).astype(jnp.int32)
        order.append(following)
    is_at = [[(order[m] == b).astype(F32) for b in range(BLOCKS)] for m in range(BLOCKS)]
    own_at = [(order[m] == blk).astype(F32) for m in range(BLOCKS)]
    block_flips = [(orient[b] == 1).astype(F32) for b in range(BLOCKS)]
    flips = [sum(is_at[m][b] * block_flips[b] for b in range(BLOCKS)) for m in range(BLOCKS)]
    own_flip = sum(own_at[m] * flips[m] for m in range(BLOCKS))

    row_id = lax.broadcasted_iota(jnp.int32, (8, MODES), 0)

    def pick(flag, yes, no):
        return yes * flag + no * (1.0 - flag)

    plane_id = lax.broadcasted_iota(jnp.int32, (BX, MODES), 0).astype(F32)
    margin_id = lax.broadcasted_iota(jnp.int32, (OV, MODES), 0).astype(F32)
    greens = []
    for h in range(HALVES):
        shift = c1 * mu_rows[...] + c2 * depth_spectrum[PLANE * h + place]
        inverse[h] = 1.0 / (c0 * jnp.concatenate([mu_planes[...]] * 2, axis=1) + shift)
        half = jnp.sqrt(shift / (4.0 * c0))
        square = half * half
        theta = 2.0 * jnp.log1p(half + square / (1.0 + jnp.sqrt(1.0 + square)))

        def power(n):
            return jnp.exp(-n * theta)

        def fall(n):
            return 1.0 - power(2.0 * n)

        scale = 1.0 / (fall(1.0) * fall(385.0))
        f64, f65, f320, f321 = fall(64.0), fall(65.0), fall(320.0), fall(321.0)
        table = {
            (0, 0): power(1.0) * f64 * f321 * scale,
            (0, 1): power(2.0) * f64 * f320 * scale,
            (0, 2): power(257.0) * f64 * f65 * scale,
            (0, 3): power(258.0) * f64 * f64 * scale,
            (1, 1): power(1.0) * f65 * f320 * scale,
            (1, 2): power(256.0) * f65 * f65 * scale,
        }
        for a, b, c, d in ((1, 3, 0, 2), (2, 2, 1, 1), (2, 3, 0, 1), (3, 3, 0, 0)):
            table[a, b] = table[c, d]
        for a in range(4):
            for b in range(a):
                table[a, b] = table[b, a]
        greens.append((table, jnp.exp(theta) * f65 / f64))
        rise = jnp.exp(-plane_id * theta)
        drop = jnp.exp((plane_id - float(BX)) * theta)
        edge = f64 * scale
        far_low = drop * power(64.0)
        far_high = rise * power(65.0)
        toward_low[h] = rise * (power(2.0) * edge) * (1.0 - far_low * far_low)
        toward_high[h] = drop * (power(1.0) * edge) * (1.0 - far_high * far_high)
        inside = jnp.exp((margin_id - float(OV)) * theta)
        margin_low[h] = jnp.exp(-margin_id * theta) * ((1.0 - inside * inside) / f64)
        outside = jnp.exp(-(margin_id + 1.0) * theta)
        margin_high[h] = jnp.exp((margin_id - float(OV - 1)) * theta) * ((1.0 - outside * outside) / f64)

    def to_ends(h, step):
        return pltpu.make_async_remote_copy(
            src_ref=ends_out.at[h],
            dst_ref=ends_in.at[h, blk],
            send_sem=ends_send.at[h, step - 1],
            recv_sem=ends_recv.at[h, step - 1],
            device_id=(wrapped(blk + step, BLOCKS), py, pz),
            device_id_type=MESH,
        )

    def summed(x):
        return jnp.sum(x, axis=0, keepdims=True)

    lane = lax.broadcasted_iota(jnp.int32, (1, 128), 1)

    def total(x):
        return jnp.sum(x, axis=1, keepdims=True)

    def norm_copy(src_ref, dst_ref, stage, step):
        device = (blk, py, wrapped(pz + step, PZ)) if stage == 0 else (blk, wrapped(py + step, PY), pz)
        return pltpu.make_async_remote_copy(
            src_ref=src_ref,
            dst_ref=dst_ref.at[pz if stage == 0 else py],
            send_sem=norm_send.at[stage, step - 1],
            recv_sem=norm_recv.at[stage, step - 1],
            device_id=device,
            device_id_type=MESH,
        )

    change_1 = jnp.zeros((1, MODES), F32)
    change_2 = jnp.zeros((1, MODES), F32)
    total_squares = jnp.zeros((1, 1), F32)
    zero = jnp.zeros((1, MODES), F32)
    def leave_ends(h):
        all_of(sent, got, go_send, go_recv, h, THERE[h]).wait_recv()
        plane = jnp.concatenate([outer_row(got, h, r, THERE[h]) for r in range(2)], axis=0)
        held = times_right(plane.T, (outer_rows[0], outer_rows[1]), NN)
        if h == 0:
            extra = times_right(row_of(got, 0, 4, THERE[0]).T, (inner_rows[0], inner_rows[1]), NN)
            for half in range(HALVES):
                for i, lane_of in enumerate((0, 127, OV, OV - 1)):
                    a, b = (lane_of + 4 * half) % 128, (lane_of + 4 * half + 2) % 128
                    extras[half, i : i + 1, :] = extra[a : a + 1, :MODES] + extra[b : b + 1, MODES:]
        at_first = extras[h, 0:1, :]
        at_last = extras[h, 1:2, :]
        cut_low = extras[h, 2:3, :] * c0
        cut_high = extras[h, 3:4, :] * c0
        held = jnp.concatenate(
            [
                held[:8] + jnp.where(row_id == 0, at_first, 0.0),
                held[8:-8],
                held[-8:] + jnp.where(row_id == 7, at_last, 0.0),
            ],
            axis=0,
        )
        near = (
            jnp.where(row_id == 0, summed(held * toward_low[h]) * (1.0 / c0), 0.0)
            + jnp.where(row_id == 1, summed(held * toward_high[h]) * (1.0 / c0), 0.0)
            + jnp.where(row_id == 2, (summed(held[:OV] * margin_low[h]) - cut_low * margin_low[h, OV - 1 : OV, :]) * (1.0 / c0), 0.0)
            + jnp.where(row_id == 3, (summed(held[BX - OV :] * margin_high[h]) - cut_high * margin_high[h, 0:1, :]) * (1.0 / c0), 0.0)
            + jnp.where(row_id == 4, own_squares, 0.0)
        )
        ends_out[h] = near
        ends_in[h, blk] = near
        for step in range(1, BLOCKS):
            to_ends(h, step).start()

        held_modes[h] = held

    def solve_own(h):
        solved_modes = times((planes_in[0], planes_in[1]), held_modes[h], NN) * inverse[h]
        base[h] = times((planes_out[0], planes_out[1]), solved_modes, NN)

    def give_back(h, total_squares, change_1, change_2):
        table, ratio = greens[h]
        for step in range(1, BLOCKS):
            to_ends(h, step).wait_recv()
        tiles = [ends_in[h, b] for b in range(BLOCKS)]
        if h == 0:
            for b in range(BLOCKS):
                total_squares = total_squares + tiles[b][4:5, :1]
        first, low, high = [], [], []
        for m in range(BLOCKS):
            at = sum(tiles[b] * is_at[m][b] for b in range(BLOCKS))
            left = pick(flips[m], at[1:2], at[0:1])
            right = pick(flips[m], at[0:1], at[1:2])
            first.append([left, left * ratio, right * ratio, right])
            low.append(pick(flips[m], at[3:4], at[2:3]))
            high.append(pick(flips[m], at[2:3], at[3:4]))
        outer = [
            [high[m - 1] if m > 0 else zero, zero, zero, low[m + 1] if m < BLOCKS - 1 else zero]
            for m in range(BLOCKS)
        ]

        def solved(m, p, sources):
            return first[m][p] + sum(table[p, q] * sources[m][q] for q in range(4))

        def jumps(sources):
            last = BLOCKS - 1
            left = [solved(m + 1, 1, sources) - solved(m, 3, sources) for m in range(last)]
            left.append(-solved(last, 3, sources))
            right = [solved(m, 2, sources) - solved(m + 1, 0, sources) for m in range(last)]
            right.append(-solved(0, 0, sources))
            return left, right

        def with_jumps(left, right):
            result = [list(o) for o in outer]
            for m in range(BLOCKS - 1):
                result[m][2] = left[m]
                result[m][3] = outer[m][3] + right[m]
                result[m + 1][1] = right[m]
                result[m + 1][0] = outer[m + 1][0] + left[m]
            result[BLOCKS - 1][2] = left[BLOCKS - 1]
            result[0][1] = right[BLOCKS - 1]
            return result

        left_1, right_1 = jumps(outer)
        left_2, right_2 = jumps(with_jumps(left_1, right_1))
        for a, b in zip(left_1 + right_1, left_2 + right_2):
            change_1 = change_1 + a * a
            change_2 = change_2 + (b - a) * (b - a)
        final = with_jumps(left_2, right_2)
        at_low = sum(own_at[m] * (final[m][0] + ratio * final[m][1]) for m in range(BLOCKS))
        at_high = sum(own_at[m] * (final[m][3] + ratio * final[m][2]) for m in range(BLOCKS))
        at_low, at_high = pick(own_flip, at_high, at_low), pick(own_flip, at_low, at_high)

        if h == HALVES - 1:
            partial = (
                jnp.where(lane == 0, total_squares, 0.0)
                + jnp.where(lane == 1, total(change_1) * (c0 * c0), 0.0)
                + jnp.where(lane == 2, total(change_2) * (c0 * c0), 0.0)
            )
            norm_out[...] = partial
            norm_x[pz] = partial
            for step in range(1, PZ):
                norm_copy(norm_out, norm_x, 0, step).start()

        across = base[h] + toward_low[h] * at_low + toward_high[h] * at_high
        plane = times((outer_rows[0], outer_rows[1]), across, NT)
        ends = [across[:1], across[-1:]]
        rim_modes = jnp.concatenate(
            [
                sum(jnp.where(row_id == 2 * r + e, ends[e], 0.0) for e in range(2))
                for r in range(2)
            ],
            axis=1,
        )
        rim_modes = jnp.concatenate([rim_modes, jnp.zeros((120, 2 * MODES), F32)], axis=0)
        for r in range(2):
            for x in range(2):
                back[h, pl.ds(2 * r + x, PLANE, stride=BACK), :] = plane[
                    PLANE * r : PLANE * (r + 1), 128 * x : 128 * (x + 1)
                ]
        back[h, pl.ds(4, PLANE, stride=BACK), :] = times((inner_rows[0], inner_rows[1]), rim_modes, NT)
        exchange(back, returned, back_send, back_recv, h, BACK)
        return total_squares, change_1, change_2

    sums = (total_squares, change_1, change_2)
    leave_ends(0)
    solve_own(0)
    leave_ends(1)
    sums = give_back(0, *sums)
    solve_own(1)
    give_back(1, *sums)

    for step in range(1, PZ):
        norm_copy(norm_out, norm_x, 0, step).wait_recv()
    partial = sum(norm_x[i] for i in range(PZ))
    norm_mid[...] = partial
    norm_z[py] = partial
    for step in range(1, PY):
        norm_copy(norm_mid, norm_z, 1, step).start()

    all_of(back, returned, back_send, back_recv, 0, BACK).wait_recv()
    for r, cells in restored(returned, 0, local, by_row, by_plane, inner, inner_back, rims, depth_out):
        partial_out[r] = cells

    for h in range(HALVES):
        all_of(sent, got, go_send, go_recv, h, THERE[h]).wait_send()
        for step in range(1, BLOCKS):
            to_ends(h, step).wait_send()
    for step in range(1, PZ):
        norm_copy(norm_out, norm_x, 0, step).wait_send()
    all_of(back, returned, back_send, back_recv, 0, BACK).wait_send()
    all_of(back, returned, back_send, back_recv, 1, BACK).wait_recv()
    for step in range(1, PY):
        norm_copy(norm_mid, norm_z, 1, step).wait_recv()
    all_of(back, returned, back_send, back_recv, 1, BACK).wait_send()
    for step in range(1, PY):
        norm_copy(norm_mid, norm_z, 1, step).wait_send()


def finish(returned, partial_out, norm_z, *refs):
    held, (out, norms, result, roots, out_sem, norm_sem) = refs[:-6], refs[-6:]
    lane = lax.broadcasted_iota(jnp.int32, (1, 128), 1)
    root = jnp.sqrt(sum(norm_z[i] for i in range(PY)) / CELLS)
    for i in range(3):
        roots[i] = jnp.sum(jnp.where(lane == i, root, 0.0))
    copies = [pltpu.make_async_copy(roots, norms, norm_sem)]
    copies[0].start()
    for r, cells in restored(returned, 1, *held):
        result[r] = partial_out[r] + cells
        copies.append(pltpu.make_async_copy(result.at[r], out.at[r], out_sem.at[r]))
        copies[-1].start()
    for copy in copies:
        copy.wait()


def shards(source, conduct, neighbours, orient):
    consts = tables()
    any_space = pl.BlockSpec(memory_space=pltpu.HBM)
    vmem = pl.BlockSpec(memory_space=pltpu.VMEM)
    dma = pltpu.SemaphoreType.DMA
    chunked = (HALVES, PLANE * BACK, 128)
    modal = (HALVES, 2 * PLANE, BX)
    cells = pltpu.VMEM((ROWS, BX, NZ), F32)
    limit = 24 * 1024 * 1024
    handed = pl.pallas_call(
        kernel,
        name="schwarz",
        out_shape=(
            jax.ShapeDtypeStruct(chunked, F32),
            jax.ShapeDtypeStruct((ROWS, BX, NZ), F32),
            jax.ShapeDtypeStruct((PY, 1, 128), F32),
            jax.ShapeDtypeStruct(modal, F32),
            jax.ShapeDtypeStruct(modal, F32),
            jax.ShapeDtypeStruct(modal, F32),
            *[jax.ShapeDtypeStruct(c.shape, BF16) for c in consts[-4:]],
        ),
        in_specs=[any_space] * (5 + len(consts)),
        out_specs=(vmem,) * 10,
        scratch_shapes=[pltpu.VMEM(c.shape, c.dtype) for c in consts[:-4]]
        + [
            pltpu.SMEM((3,), F32),
            pltpu.SMEM((2, BLOCKS), jnp.int32),
            pltpu.SMEM((BLOCKS,), jnp.int32),
            pltpu.SMEM((NZ,), F32),
            cells,
            pltpu.VMEM(chunked, F32),
            pltpu.VMEM(chunked, F32),
            pltpu.VMEM((HALVES, BX, MODES), F32),
            pltpu.VMEM((HALVES, 8, MODES), F32),
            pltpu.VMEM((HALVES, BX, MODES), F32),
            pltpu.VMEM((HALVES, EXT, MODES), F32),
            pltpu.VMEM((HALVES, BX, MODES), F32),
            pltpu.VMEM((HALVES, BX, MODES), F32),
            pltpu.VMEM((HALVES, OV, MODES), F32),
            pltpu.VMEM((HALVES, OV, MODES), F32),
            pltpu.VMEM((HALVES, 8, MODES), F32),
            pltpu.VMEM((HALVES, BLOCKS, 8, MODES), F32),
            pltpu.VMEM(chunked, F32),
            pltpu.VMEM((1, 128), F32),
            pltpu.VMEM((PZ, 1, 128), F32),
            pltpu.VMEM((1, 128), F32),
            dma((ROWS,)),
            dma((len(consts),)),
            dma((4,)),
            dma((HALVES,)),
            dma((HALVES,)),
            dma((HALVES, BLOCKS - 1)),
            dma((HALVES, BLOCKS - 1)),
            dma((HALVES,)),
            dma((HALVES,)),
            dma((2, PZ - 1)),
            dma((2, PZ - 1)),
        ],
        compiler_params=pltpu.CompilerParams(collective_id=0, has_side_effects=True, vmem_limit_bytes=limit),
    )(
        *[
            pltpu.with_memory_space_constraint(jnp.asarray(a), pltpu.HBM)
            for a in (
                source,
                conduct,
                neighbours.T,
                orient,
                eigenvalues(NZ).astype(np.float32),
                *consts,
            )
        ]
    )
    return pl.pallas_call(
        finish,
        name="finish",
        out_shape=(
            jax.ShapeDtypeStruct((ROWS, BX, NZ), F32),
            jax.ShapeDtypeStruct((3,), F32),
        ),
        in_specs=[vmem] * 10,
        out_specs=(any_space, any_space),
        scratch_shapes=[cells, pltpu.SMEM((3,), F32), dma((ROWS,)), dma],
        compiler_params=pltpu.CompilerParams(vmem_limit_bytes=limit),
    )(*handed)


def solution(mesh):
    cells = P(("py", "pz"), "blk", None)
    return jax.shard_map(
        shards, mesh=mesh, in_specs=(cells, P(), P(), P()), out_specs=(cells, P()), check_vma=False
    )
```

```python
import functools

import jax
import jax.numpy as jnp
import ml_dtypes
import numpy as np
from jax import lax
from jax.experimental import pallas as pl
from jax.experimental.pallas import tpu as pltpu
from jax.sharding import PartitionSpec as P

NY = 256
NZ = 128
BX = 256
OV = 64
EXT = 384
BLOCKS = 4
PY = 8
PZ = 8
PLANE = PY * PZ
ROWS = NY // PLANE
HALVES = 2
MODES = 256
MESH = pl.DeviceIdType.MESH
F32 = jnp.float32
BF16 = jnp.bfloat16
NN = (((1,), (0,)), ((), ()))
NT = (((1,), (1,)), ((), ()))
CELLS = float(BLOCKS * BX * NY * NZ)
TN = (((0,), (0,)), ((), ()))
BACK = 5
THERE = (5, 4)
CONSTS = 13
EARLY = 3


def basis(n):
    j = np.arange(1, n + 1)
    m = (j[:, None] * j[None, :]) % (2 * (n + 1))
    return np.sqrt(2.0 / (n + 1)) * np.sin(np.pi * m / (n + 1))


def eigenvalues(n):
    return 4.0 * np.sin(np.pi * np.arange(1, n + 1) / (2.0 * (n + 1))) ** 2


def halves(a):
    a = a.astype(np.float32)
    hi = a.astype(ml_dtypes.bfloat16)
    lo = (a - hi.astype(np.float32)).astype(ml_dtypes.bfloat16)
    return np.stack([hi, lo])


@functools.lru_cache(None)
def tables():
    depth = halves(basis(NZ))
    rows = basis(NY)
    planes = basis(EXT)
    first = ROWS * np.arange(PLANE)
    outer_rows = rows[np.concatenate([first, first + ROWS - 1])]
    inner_rows = np.concatenate([rows[first + 1], rows[first + 2]], axis=1)
    inner = np.zeros((BX, BX))
    inner[1:-1, :-2] = basis(BX - 2)
    mu_inner = np.concatenate([eigenvalues(BX - 2), np.ones(2)])[None, :]
    rims = np.zeros((128, 2 * BX))
    rims[:4] = np.concatenate(
        [np.stack([inner[1], inner[-2]] * 2), np.stack([inner[1], inner[-2], -inner[1], -inner[-2]])], axis=1
    )
    planes_in = planes[OV : OV + BX].T
    depth_in = np.concatenate([depth[0], depth[0], depth[1]], axis=1)
    depth_out = np.stack(
        [
            np.concatenate([part[PLANE * h : PLANE * (h + 1)] for part in (depth[0], depth[0], depth[1])], axis=0)
            for h in range(HALVES)
        ]
    )
    return (
        depth_in,
        mu_inner.astype(np.float32),
        (eigenvalues(NZ)[:, None] * np.ones((1, 128))).astype(np.float32),
        halves(outer_rows),
        halves(inner_rows),
        halves(planes_in),
        halves(planes_in.T),
        (eigenvalues(EXT)[:, None] * np.ones((1, 128))).astype(np.float32),
        eigenvalues(NY)[None, :].astype(np.float32),
        halves(inner),
        halves(inner.T),
        halves(rims),
        depth_out,
    )


def split(x):
    hi = x.astype(BF16)
    return hi, (x - hi.astype(F32)).astype(BF16)


def dot(a, b, dims):
    return lax.dot_general(a, b, dimension_numbers=dims, preferred_element_type=F32)


def times(table, x, dims):
    hi, lo = split(x)
    return dot(table[0], hi, dims) + (dot(table[0], lo, dims) + dot(table[1], hi, dims))


def times_right(x, table, dims):
    hi, lo = split(x)
    return dot(hi, table[0], dims) + (dot(lo, table[0], dims) + dot(hi, table[1], dims))


def row_of(ref, h, slot, slots):
    return ref[h, pl.ds(slot, PLANE, stride=slots), :]


def outer_row(ref, h, r, slots):
    return jnp.concatenate([row_of(ref, h, 2 * r + x, slots) for x in range(2)], axis=1)


def restored(returned, h, local, by_row, by_plane, inner, inner_back, rims, depth_out):
    low_row = outer_row(returned, h, 0, BACK)
    high_row = outer_row(returned, h, 1, BACK)
    yield 0, depth_back(low_row, depth_out[h])
    yield 3, depth_back(high_row, depth_out[h])
    rim = row_of(returned, h, 4, BACK)
    from_rows = times_right(
        jnp.concatenate([low_row + high_row, low_row - high_row], axis=0), (inner[0], inner[1]), NN
    )
    from_rim = times_right(rim, (rims[0], rims[1]), NN)
    from_rim = jnp.concatenate([from_rim[:, :BX], from_rim[:, BX:]], axis=0)
    both = times_right(
        local[h] + by_row[h] * from_rows + by_plane[h] * from_rim, (inner_back[0], inner_back[1]), NN
    )
    plane = lax.broadcasted_iota(jnp.int32, (PLANE, BX), 1)

    def edged(cells, slot):
        cells = jnp.where(plane == 0, rim[:, slot : slot + 1], cells)
        return jnp.where(plane == BX - 1, rim[:, slot + 1 : slot + 2], cells)

    even, odd = both[:PLANE], both[PLANE:]
    yield 1, depth_back(edged(even + odd, 0), depth_out[h])
    yield 2, depth_back(edged(even - odd, 2), depth_out[h])


def depth_back(cells, table):
    hi, lo = split(cells)
    return dot(jnp.concatenate([hi, lo, hi], axis=0), table, TN)


def kernel(source, conduct_hbm, neighbours_hbm, orient_hbm, spectrum_hbm, *refs):
    consts_hbm = refs[:CONSTS]
    returned, partial_out, norm_z, local, by_row, by_plane, inner, inner_back, rims, depth_out = refs[
        CONSTS : CONSTS + 10
    ]
    consts = refs[CONSTS + 10 : 2 * CONSTS + 6] + (inner, inner_back, rims, depth_out)
    (
        conduct,
        neighbours,
        orient,
        depth_spectrum,
        src,
        sent,
        got,
        held_modes,
        extras,
        base,
        inverse,
        toward_low,
        toward_high,
        margin_low,
        margin_high,
        ends_out,
        ends_in,
        back,
        norm_out,
        norm_x,
        norm_mid,
        src_sem,
        const_sem,
        small_sem,
        go_send,
        go_recv,
        ends_send,
        ends_recv,
        back_send,
        back_recv,
        norm_send,
        norm_recv,
    ) = refs[2 * CONSTS + 6 :]
    depth_in, mu_inner, mu_depth, outer_rows, inner_rows, planes_in, planes_out, mu_planes, mu_rows = consts[:9]

    blk = lax.axis_index("blk")
    py = lax.axis_index("py")
    pz = lax.axis_index("pz")
    place = py * PZ + pz

    def wrapped(a, n):
        return jnp.where(a >= n, a - n, a)

    core = lax.rem(pz, 2)
    chip = pz // 2

    def everyone(visit, first_core):
        def one(near, to_pz):
            to_py = wrapped(py + near, PY)
            visit(to_py, to_pz, to_py * PZ + to_pz)

        def group(turn, carry):
            to_core = turn if first_core == 0 else 1 - turn
            for far in (2, 1, 3):
                for near in (4, 3, 5, 2, 6, 1, 7, 0):
                    one(near, wrapped(chip + far, PZ // 2) * 2 + to_core)
            for near in (4, 3, 5, 2, 6, 1, 7):
                one(near, chip * 2 + to_core)
            return carry

        one(0, chip * 2 + 1 - core)
        lax.fori_loop(0, 2, group, 0)

    barrier = pltpu.get_barrier_semaphore()

    def greet(to_py, to_pz, to):
        pl.semaphore_signal(barrier, inc=1, device_id=(blk, to_py, to_pz), device_id_type=MESH)

    loads = [pltpu.make_async_copy(source.at[y], src.at[y], src_sem.at[y]) for y in range(ROWS)]
    fetches = [pltpu.make_async_copy(a, b, const_sem.at[i]) for i, (a, b) in enumerate(zip(consts_hbm, consts))]
    smalls = [
        pltpu.make_async_copy(a, b, small_sem.at[i])
        for i, (a, b) in enumerate(
            (
                (conduct_hbm, conduct),
                (neighbours_hbm, neighbours),
                (orient_hbm, orient),
                (spectrum_hbm, depth_spectrum),
            )
        )
    ]
    early = fetches[:EARLY] + fetches[9:11]
    late = fetches[EARLY:9] + fetches[11:]
    everyone(greet, 0)
    for start in smalls + loads + early:
        start.start()
    for step in range(1, BLOCKS):
        pl.semaphore_signal(
            barrier, inc=1, device_id=(wrapped(blk + step, BLOCKS), py, pz), device_id_type=MESH
        )
    for fetch in late:
        fetch.start()

    fetches[0].wait()
    squares = jnp.zeros((8, 128), F32)
    rows = []
    for y in range(ROWS):
        loads[y].wait()
        cells = src[y]
        squares = squares + jnp.sum((cells * cells).reshape(BX // 8, 8, NZ), axis=0)
        hi, lo = split(cells)
        rows.append(dot(depth_in[...], jnp.concatenate([hi, lo, hi], axis=1), NT))
    own_squares = jnp.sum(jnp.sum(squares, axis=0, keepdims=True), axis=1, keepdims=True)

    for wait in smalls + early[1:]:
        wait.wait()
    c0 = conduct[0]
    c1 = conduct[1]
    c2 = conduct[2]

    base_part = c0 * mu_inner[...] + c2 * jnp.concatenate([mu_depth[...]] * 2, axis=1)
    weights = jnp.concatenate([0.5 / (base_part + c1), 0.5 / (base_part + 3.0 * c1)], axis=0)
    mixed = jnp.concatenate([rows[1] + rows[2], rows[1] - rows[2]], axis=0)
    inner_modes = times_right(mixed, (inner[0], inner[1]), NN) * weights
    for h in range(HALVES):
        own = [slice(NZ * q + PLANE * h, NZ * q + PLANE * (h + 1)) for q in range(2)]
        weight = jnp.concatenate([weights[part] for part in own], axis=0)
        local[h] = jnp.concatenate([inner_modes[part] for part in own], axis=0)
        by_row[h] = weight * c1
        by_plane[h] = weight * c0
    both = times_right(inner_modes, (inner_back[0], inner_back[1]), NN)
    solved_rows = (both[:NZ] + both[NZ:], both[:NZ] - both[NZ:])
    lanes = lax.broadcasted_iota(jnp.int32, (NZ, 128), 1)
    rim = jnp.zeros((NZ, 128), F32)
    for r in range(2):
        near, far = solved_rows[r][:, :128], solved_rows[r][:, 128:]
        at_first = rows[1 + r][:, :128] + c0 * pltpu.roll(near, 127, 1)
        at_last = rows[1 + r][:, 128:] + c0 * pltpu.roll(far, 1, 1)
        part = jnp.where(lanes == 0, at_first, 0.0)
        part = jnp.where(lanes == 127, at_last, part)
        part = jnp.where(lanes == OV, near, part)
        part = jnp.where(lanes == OV - 1, far, part)
        rim = rim + (part if r == 0 else pltpu.roll(part, 2, 1))
    outer_cells = (rows[0] + c1 * solved_rows[0], rows[3] + c1 * solved_rows[1])
    for h in range(HALVES):
        part = slice(PLANE * h, PLANE * (h + 1))
        for r in range(2):
            for x in range(2):
                sent[h, pl.ds(2 * r + x, PLANE, stride=THERE[h]), :] = outer_cells[r][
                    part, 128 * x : 128 * (x + 1)
                ]
    sent[0, pl.ds(4, PLANE, stride=THERE[0]), :] = rim[:PLANE] + pltpu.roll(rim[PLANE:], 4, 1)

    pl.semaphore_wait(barrier, PLANE - 1 + BLOCKS - 1)

    def exchange(src_ref, dst_ref, send_sem, recv_sem, h, slots, first_core):
        def tile(d):
            return pl.ds(d * slots, slots)

        def send(to_py, to_pz, to):
            pltpu.make_async_remote_copy(
                src_ref=src_ref.at[h, tile(to), :],
                dst_ref=dst_ref.at[h, tile(place), :],
                send_sem=send_sem.at[h],
                recv_sem=recv_sem.at[h],
                device_id=(blk, to_py, to_pz),
                device_id_type=MESH,
            ).start()

        everyone(send, first_core)
        dst_ref[h, tile(place), :] = src_ref[h, tile(place), :]

    def all_of(src_ref, dst_ref, send_sem, recv_sem, h, slots):
        others = pl.ds(0, (PLANE - 1) * slots)
        return pltpu.make_async_remote_copy(
            src_ref=src_ref.at[h, others, :],
            dst_ref=dst_ref.at[h, others, :],
            send_sem=send_sem.at[h],
            recv_sem=recv_sem.at[h],
            device_id=(blk, wrapped(py + 1, PY), pz),
            device_id_type=MESH,
        )

    for h in range(HALVES):
        exchange(sent, got, go_send, go_recv, h, THERE[h], 0)

    for fetch in late:
        fetch.wait()

    order = [jnp.int32(0)]
    for b in range(BLOCKS):
        order[0] = order[0] + b * (neighbours[0, b] == -1).astype(jnp.int32)
    for m in range(1, BLOCKS):
        following = jnp.int32(0)
        for b in range(BLOCKS):
            following = following + neighbours[1, b] * (order[m - 1] == b).astype(jnp.int32)
        order.append(following)
    is_at = [[(order[m] == b).astype(F32) for b in range(BLOCKS)] for m in range(BLOCKS)]
    own_at = [(order[m] == blk).astype(F32) for m in range(BLOCKS)]
    block_flips = [(orient[b] == 1).astype(F32) for b in range(BLOCKS)]
    flips = [sum(is_at[m][b] * block_flips[b] for b in range(BLOCKS)) for m in range(BLOCKS)]
    own_flip = sum(own_at[m] * flips[m] for m in range(BLOCKS))

    row_id = lax.broadcasted_iota(jnp.int32, (8, MODES), 0)

    def pick(flag, yes, no):
        return yes * flag + no * (1.0 - flag)

    plane_id = lax.broadcasted_iota(jnp.int32, (BX, MODES), 0).astype(F32)
    margin_id = lax.broadcasted_iota(jnp.int32, (OV, MODES), 0).astype(F32)
    greens = []
    for h in range(HALVES):
        shift = c1 * mu_rows[...] + c2 * depth_spectrum[PLANE * h + place]
        inverse[h] = 1.0 / (c0 * jnp.concatenate([mu_planes[...]] * 2, axis=1) + shift)
        half = jnp.sqrt(shift / (4.0 * c0))
        square = half * half
        theta = 2.0 * jnp.log1p(half + square / (1.0 + jnp.sqrt(1.0 + square)))

        def power(n):
            return jnp.exp(-n * theta)

        def fall(n):
            return 1.0 - power(2.0 * n)

        scale = 1.0 / (fall(1.0) * fall(385.0))
        f64, f65, f320, f321 = fall(64.0), fall(65.0), fall(320.0), fall(321.0)
        table = {
            (0, 0): power(1.0) * f64 * f321 * scale,
            (0, 1): power(2.0) * f64 * f320 * scale,
            (0, 2): power(257.0) * f64 * f65 * scale,
            (0, 3): power(258.0) * f64 * f64 * scale,
            (1, 1): power(1.0) * f65 * f320 * scale,
            (1, 2): power(256.0) * f65 * f65 * scale,
        }
        for a, b, c, d in ((1, 3, 0, 2), (2, 2, 1, 1), (2, 3, 0, 1), (3, 3, 0, 0)):
            table[a, b] = table[c, d]
        for a in range(4):
            for b in range(a):
                table[a, b] = table[b, a]
        greens.append((table, jnp.exp(theta) * f65 / f64))
        rise = jnp.exp(-plane_id * theta)
        drop = jnp.exp((plane_id - float(BX)) * theta)
        edge = f64 * scale
        far_low = drop * power(64.0)
        far_high = rise * power(65.0)
        toward_low[h] = rise * (power(2.0) * edge) * (1.0 - far_low * far_low)
        toward_high[h] = drop * (power(1.0) * edge) * (1.0 - far_high * far_high)
        inside = jnp.exp((margin_id - float(OV)) * theta)
        margin_low[h] = jnp.exp(-margin_id * theta) * ((1.0 - inside * inside) / f64)
        outside = jnp.exp(-(margin_id + 1.0) * theta)
        margin_high[h] = jnp.exp((margin_id - float(OV - 1)) * theta) * ((1.0 - outside * outside) / f64)

    def to_ends(h, step):
        return pltpu.make_async_remote_copy(
            src_ref=ends_out.at[h],
            dst_ref=ends_in.at[h, blk],
            send_sem=ends_send.at[h, step - 1],
            recv_sem=ends_recv.at[h, step - 1],
            device_id=(wrapped(blk + step, BLOCKS), py, pz),
            device_id_type=MESH,
        )

    def summed(x):
        return jnp.sum(x, axis=0, keepdims=True)

    lane = lax.broadcasted_iota(jnp.int32, (1, 128), 1)

    def total(x):
        return jnp.sum(x, axis=1, keepdims=True)

    def norm_copy(src_ref, dst_ref, stage, step):
        device = (blk, py, wrapped(pz + step, PZ)) if stage == 0 else (blk, wrapped(py + step, PY), pz)
        return pltpu.make_async_remote_copy(
            src_ref=src_ref,
            dst_ref=dst_ref.at[pz if stage == 0 else py],
            send_sem=norm_send.at[stage, step - 1],
            recv_sem=norm_recv.at[stage, step - 1],
            device_id=device,
            device_id_type=MESH,
        )

    change_1 = jnp.zeros((1, MODES), F32)
    change_2 = jnp.zeros((1, MODES), F32)
    total_squares = jnp.zeros((1, 1), F32)
    zero = jnp.zeros((1, MODES), F32)
    def leave_ends(h):
        all_of(sent, got, go_send, go_recv, h, THERE[h]).wait_recv()
        plane = jnp.concatenate([outer_row(got, h, r, THERE[h]) for r in range(2)], axis=0)
        held = times_right(plane.T, (outer_rows[0], outer_rows[1]), NN)
        if h == 0:
            extra = times_right(row_of(got, 0, 4, THERE[0]).T, (inner_rows[0], inner_rows[1]), NN)
            for half in range(HALVES):
                for i, lane_of in enumerate((0, 127, OV, OV - 1)):
                    a, b = (lane_of + 4 * half) % 128, (lane_of + 4 * half + 2) % 128
                    extras[half, i : i + 1, :] = extra[a : a + 1, :MODES] + extra[b : b + 1, MODES:]
        at_first = extras[h, 0:1, :]
        at_last = extras[h, 1:2, :]
        cut_low = extras[h, 2:3, :] * c0
        cut_high = extras[h, 3:4, :] * c0
        held = jnp.concatenate(
            [
                held[:8] + jnp.where(row_id == 0, at_first, 0.0),
                held[8:-8],
                held[-8:] + jnp.where(row_id == 7, at_last, 0.0),
            ],
            axis=0,
        )
        near = (
            jnp.where(row_id == 0, summed(held * toward_low[h]) * (1.0 / c0), 0.0)
            + jnp.where(row_id == 1, summed(held * toward_high[h]) * (1.0 / c0), 0.0)
            + jnp.where(row_id == 2, (summed(held[:OV] * margin_low[h]) - cut_low * margin_low[h, OV - 1 : OV, :]) * (1.0 / c0), 0.0)
            + jnp.where(row_id == 3, (summed(held[BX - OV :] * margin_high[h]) - cut_high * margin_high[h, 0:1, :]) * (1.0 / c0), 0.0)
            + jnp.where(row_id == 4, own_squares, 0.0)
        )
        ends_out[h] = near
        ends_in[h, blk] = near
        for step in range(1, BLOCKS):
            to_ends(h, step).start()

        held_modes[h] = held

    def solve_own(h):
        solved_modes = times((planes_in[0], planes_in[1]), held_modes[h], NN) * inverse[h]
        base[h] = times((planes_out[0], planes_out[1]), solved_modes, NN)

    def give_back(h, total_squares, change_1, change_2):
        table, ratio = greens[h]
        for step in range(1, BLOCKS):
            to_ends(h, step).wait_recv()
        tiles = [ends_in[h, b] for b in range(BLOCKS)]
        if h == 0:
            for b in range(BLOCKS):
                total_squares = total_squares + tiles[b][4:5, :1]
        first, low, high = [], [], []
        for m in range(BLOCKS):
            at = sum(tiles[b] * is_at[m][b] for b in range(BLOCKS))
            left = pick(flips[m], at[1:2], at[0:1])
            right = pick(flips[m], at[0:1], at[1:2])
            first.append([left, left * ratio, right * ratio, right])
            low.append(pick(flips[m], at[3:4], at[2:3]))
            high.append(pick(flips[m], at[2:3], at[3:4]))
        outer = [
            [high[m - 1] if m > 0 else zero, zero, zero, low[m + 1] if m < BLOCKS - 1 else zero]
            for m in range(BLOCKS)
        ]

        def solved(m, p, sources):
            return first[m][p] + sum(table[p, q] * sources[m][q] for q in range(4))

        def jumps(sources):
            last = BLOCKS - 1
            left = [solved(m + 1, 1, sources) - solved(m, 3, sources) for m in range(last)]
            left.append(-solved(last, 3, sources))
            right = [solved(m, 2, sources) - solved(m + 1, 0, sources) for m in range(last)]
            right.append(-solved(0, 0, sources))
            return left, right

        def with_jumps(left, right):
            result = [list(o) for o in outer]
            for m in range(BLOCKS - 1):
                result[m][2] = left[m]
                result[m][3] = outer[m][3] + right[m]
                result[m + 1][1] = right[m]
                result[m + 1][0] = outer[m + 1][0] + left[m]
            result[BLOCKS - 1][2] = left[BLOCKS - 1]
            result[0][1] = right[BLOCKS - 1]
            return result

        left_1, right_1 = jumps(outer)
        left_2, right_2 = jumps(with_jumps(left_1, right_1))
        for a, b in zip(left_1 + right_1, left_2 + right_2):
            change_1 = change_1 + a * a
            change_2 = change_2 + (b - a) * (b - a)
        final = with_jumps(left_2, right_2)
        at_low = sum(own_at[m] * (final[m][0] + ratio * final[m][1]) for m in range(BLOCKS))
        at_high = sum(own_at[m] * (final[m][3] + ratio * final[m][2]) for m in range(BLOCKS))
        at_low, at_high = pick(own_flip, at_high, at_low), pick(own_flip, at_low, at_high)

        if h == HALVES - 1:
            partial = (
                jnp.where(lane == 0, total_squares, 0.0)
                + jnp.where(lane == 1, total(change_1) * (c0 * c0), 0.0)
                + jnp.where(lane == 2, total(change_2) * (c0 * c0), 0.0)
            )
            norm_out[...] = partial
            norm_x[pz] = partial
            for step in range(1, PZ):
                norm_copy(norm_out, norm_x, 0, step).start()

        across = base[h] + toward_low[h] * at_low + toward_high[h] * at_high
        plane = times((outer_rows[0], outer_rows[1]), across, NT)
        ends = [across[:1], across[-1:]]
        rim_modes = jnp.concatenate(
            [
                sum(jnp.where(row_id == 2 * r + e, ends[e], 0.0) for e in range(2))
                for r in range(2)
            ],
            axis=1,
        )
        rim_modes = jnp.concatenate([rim_modes, jnp.zeros((120, 2 * MODES), F32)], axis=0)
        for r in range(2):
            for x in range(2):
                back[h, pl.ds(2 * r + x, PLANE, stride=BACK), :] = plane[
                    PLANE * r : PLANE * (r + 1), 128 * x : 128 * (x + 1)
                ]
        back[h, pl.ds(4, PLANE, stride=BACK), :] = times((inner_rows[0], inner_rows[1]), rim_modes, NT)
        exchange(back, returned, back_send, back_recv, h, BACK, 1)
        return total_squares, change_1, change_2

    sums = (total_squares, change_1, change_2)
    leave_ends(0)
    solve_own(0)
    leave_ends(1)
    sums = give_back(0, *sums)
    solve_own(1)
    give_back(1, *sums)

    for step in range(1, PZ):
        norm_copy(norm_out, norm_x, 0, step).wait_recv()
    partial = sum(norm_x[i] for i in range(PZ))
    norm_mid[...] = partial
    norm_z[py] = partial
    for step in range(1, PY):
        norm_copy(norm_mid, norm_z, 1, step).start()

    all_of(back, returned, back_send, back_recv, 0, BACK).wait_recv()
    for r, cells in restored(returned, 0, local, by_row, by_plane, inner, inner_back, rims, depth_out):
        partial_out[r] = cells

    for h in range(HALVES):
        all_of(sent, got, go_send, go_recv, h, THERE[h]).wait_send()
        for step in range(1, BLOCKS):
            to_ends(h, step).wait_send()
    for step in range(1, PZ):
        norm_copy(norm_out, norm_x, 0, step).wait_send()
    all_of(back, returned, back_send, back_recv, 0, BACK).wait_send()
    all_of(back, returned, back_send, back_recv, 1, BACK).wait_recv()
    for step in range(1, PY):
        norm_copy(norm_mid, norm_z, 1, step).wait_recv()
    all_of(back, returned, back_send, back_recv, 1, BACK).wait_send()
    for step in range(1, PY):
        norm_copy(norm_mid, norm_z, 1, step).wait_send()


def finish(returned, partial_out, norm_z, *refs):
    held, (out, norms, result, roots, out_sem, norm_sem) = refs[:-6], refs[-6:]
    lane = lax.broadcasted_iota(jnp.int32, (1, 128), 1)
    root = jnp.sqrt(sum(norm_z[i] for i in range(PY)) / CELLS)
    for i in range(3):
        roots[i] = jnp.sum(jnp.where(lane == i, root, 0.0))
    copies = [pltpu.make_async_copy(roots, norms, norm_sem)]
    copies[0].start()
    for r, cells in restored(returned, 1, *held):
        result[r] = partial_out[r] + cells
        copies.append(pltpu.make_async_copy(result.at[r], out.at[r], out_sem.at[r]))
        copies[-1].start()
    for copy in copies:
        copy.wait()


def shards(source, conduct, neighbours, orient):
    consts = tables()
    any_space = pl.BlockSpec(memory_space=pltpu.HBM)
    vmem = pl.BlockSpec(memory_space=pltpu.VMEM)
    dma = pltpu.SemaphoreType.DMA
    chunked = (HALVES, PLANE * BACK, 128)
    modal = (HALVES, 2 * PLANE, BX)
    cells = pltpu.VMEM((ROWS, BX, NZ), F32)
    limit = 24 * 1024 * 1024
    handed = pl.pallas_call(
        kernel,
        name="schwarz",
        out_shape=(
            jax.ShapeDtypeStruct(chunked, F32),
            jax.ShapeDtypeStruct((ROWS, BX, NZ), F32),
            jax.ShapeDtypeStruct((PY, 1, 128), F32),
            jax.ShapeDtypeStruct(modal, F32),
            jax.ShapeDtypeStruct(modal, F32),
            jax.ShapeDtypeStruct(modal, F32),
            *[jax.ShapeDtypeStruct(c.shape, BF16) for c in consts[-4:]],
        ),
        in_specs=[any_space] * (5 + len(consts)),
        out_specs=(vmem,) * 10,
        scratch_shapes=[pltpu.VMEM(c.shape, c.dtype) for c in consts[:-4]]
        + [
            pltpu.SMEM((3,), F32),
            pltpu.SMEM((2, BLOCKS), jnp.int32),
            pltpu.SMEM((BLOCKS,), jnp.int32),
            pltpu.SMEM((NZ,), F32),
            cells,
            pltpu.VMEM(chunked, F32),
            pltpu.VMEM(chunked, F32),
            pltpu.VMEM((HALVES, BX, MODES), F32),
            pltpu.VMEM((HALVES, 8, MODES), F32),
            pltpu.VMEM((HALVES, BX, MODES), F32),
            pltpu.VMEM((HALVES, EXT, MODES), F32),
            pltpu.VMEM((HALVES, BX, MODES), F32),
            pltpu.VMEM((HALVES, BX, MODES), F32),
            pltpu.VMEM((HALVES, OV, MODES), F32),
            pltpu.VMEM((HALVES, OV, MODES), F32),
            pltpu.VMEM((HALVES, 8, MODES), F32),
            pltpu.VMEM((HALVES, BLOCKS, 8, MODES), F32),
            pltpu.VMEM(chunked, F32),
            pltpu.VMEM((1, 128), F32),
            pltpu.VMEM((PZ, 1, 128), F32),
            pltpu.VMEM((1, 128), F32),
            dma((ROWS,)),
            dma((len(consts),)),
            dma((4,)),
            dma((HALVES,)),
            dma((HALVES,)),
            dma((HALVES, BLOCKS - 1)),
            dma((HALVES, BLOCKS - 1)),
            dma((HALVES,)),
            dma((HALVES,)),
            dma((2, PZ - 1)),
            dma((2, PZ - 1)),
        ],
        compiler_params=pltpu.CompilerParams(collective_id=0, has_side_effects=True, vmem_limit_bytes=limit),
    )(
        *[
            pltpu.with_memory_space_constraint(jnp.asarray(a), pltpu.HBM)
            for a in (
                source,
                conduct,
                neighbours.T,
                orient,
                eigenvalues(NZ).astype(np.float32),
                *consts,
            )
        ]
    )
    return pl.pallas_call(
        finish,
        name="finish",
        out_shape=(
            jax.ShapeDtypeStruct((ROWS, BX, NZ), F32),
            jax.ShapeDtypeStruct((3,), F32),
        ),
        in_specs=[vmem] * 10,
        out_specs=(any_space, any_space),
        scratch_shapes=[cells, pltpu.SMEM((3,), F32), dma((ROWS,)), dma],
        compiler_params=pltpu.CompilerParams(vmem_limit_bytes=limit),
    )(*handed)


def solution(mesh):
    cells = P(("py", "pz"), "blk", None)
    return jax.shard_map(
        shards, mesh=mesh, in_specs=(cells, P(), P(), P()), out_specs=(cells, P()), check_vma=False
    )
```

```python
import functools

import jax
import jax.numpy as jnp
import ml_dtypes
import numpy as np
from jax import lax
from jax.experimental import pallas as pl
from jax.experimental.pallas import tpu as pltpu
from jax.sharding import PartitionSpec as P

NY = 256
NZ = 128
BX = 256
OV = 64
EXT = 384
BLOCKS = 4
PY = 8
PZ = 8
PLANE = PY * PZ
ROWS = NY // PLANE
HALVES = 2
MODES = 256
MESH = pl.DeviceIdType.MESH
F32 = jnp.float32
BF16 = jnp.bfloat16
NN = (((1,), (0,)), ((), ()))
NT = (((1,), (1,)), ((), ()))
CELLS = float(BLOCKS * BX * NY * NZ)
TN = (((0,), (0,)), ((), ()))
BACK = (4, 5)
THERE = (5, 4)
CONSTS = 13
EARLY = 3


def basis(n):
    j = np.arange(1, n + 1)
    m = (j[:, None] * j[None, :]) % (2 * (n + 1))
    return np.sqrt(2.0 / (n + 1)) * np.sin(np.pi * m / (n + 1))


def eigenvalues(n):
    return 4.0 * np.sin(np.pi * np.arange(1, n + 1) / (2.0 * (n + 1))) ** 2


def halves(a):
    a = a.astype(np.float32)
    hi = a.astype(ml_dtypes.bfloat16)
    lo = (a - hi.astype(np.float32)).astype(ml_dtypes.bfloat16)
    return np.stack([hi, lo])


@functools.lru_cache(None)
def tables():
    depth = halves(basis(NZ))
    rows = basis(NY)
    planes = basis(EXT)
    first = ROWS * np.arange(PLANE)
    outer_rows = rows[np.concatenate([first, first + ROWS - 1])]
    inner_rows = np.concatenate([rows[first + 1], rows[first + 2]], axis=1)
    inner = np.zeros((BX, BX))
    inner[1:-1, :-2] = basis(BX - 2)
    mu_inner = np.concatenate([eigenvalues(BX - 2), np.ones(2)])[None, :]
    rims = np.zeros((8, HALVES * 2 * BX))
    for h in range(HALVES):
        columns = slice(2 * BX * h, 2 * BX * (h + 1))
        rims[4 * h : 4 * h + 4, columns] = np.concatenate(
            [np.stack([inner[1], inner[-2]] * 2), np.stack([inner[1], inner[-2], -inner[1], -inner[-2]])], axis=1
        )
    planes_in = planes[OV : OV + BX].T
    depth_in = np.concatenate([depth[0], depth[0], depth[1]], axis=1)
    depth_out = np.stack(
        [
            np.concatenate([part[PLANE * h : PLANE * (h + 1)] for part in (depth[0], depth[0], depth[1])], axis=0)
            for h in range(HALVES)
        ]
    )
    return (
        depth_in,
        mu_inner.astype(np.float32),
        (eigenvalues(NZ)[:, None] * np.ones((1, 128))).astype(np.float32),
        halves(outer_rows),
        halves(inner_rows),
        halves(planes_in),
        halves(planes_in.T),
        (eigenvalues(EXT)[:, None] * np.ones((1, 128))).astype(np.float32),
        eigenvalues(NY)[None, :].astype(np.float32),
        halves(inner),
        halves(inner.T),
        halves(rims),
        depth_out,
    )


def split(x):
    hi = x.astype(BF16)
    return hi, (x - hi.astype(F32)).astype(BF16)


def dot(a, b, dims):
    return lax.dot_general(a, b, dimension_numbers=dims, preferred_element_type=F32)


def times(table, x, dims):
    hi, lo = split(x)
    return dot(table[0], hi, dims) + (dot(table[0], lo, dims) + dot(table[1], hi, dims))


def times_right(x, table, dims):
    hi, lo = split(x)
    return dot(hi, table[0], dims) + (dot(lo, table[0], dims) + dot(hi, table[1], dims))


def row_of(ref, h, slot, slots):
    return ref[h, pl.ds(slot, PLANE, stride=slots), :]


def outer_row(ref, h, r, slots):
    return jnp.concatenate([row_of(ref, h, 2 * r + x, slots) for x in range(2)], axis=1)


def outer_restored(returned, h, depth_out):
    low_row = outer_row(returned, h, 0, BACK[h])
    high_row = outer_row(returned, h, 1, BACK[h])
    mixed = jnp.concatenate([low_row + high_row, low_row - high_row], axis=0)
    return depth_back(low_row, depth_out[h]), depth_back(high_row, depth_out[h]), mixed


def rows_of(both):
    return both[:PLANE] + both[PLANE:], both[:PLANE] - both[PLANE:]


def depth_back(cells, table):
    hi, lo = split(cells)
    return dot(jnp.concatenate([hi, lo, hi], axis=0), table, TN)


def kernel(source, conduct_hbm, neighbours_hbm, orient_hbm, spectrum_hbm, *refs):
    consts_hbm = refs[:CONSTS]
    returned, partial_out, norm_z, local, by_row, by_plane, inner, inner_back, rims, depth_out = refs[
        CONSTS : CONSTS + 10
    ]
    consts = refs[CONSTS + 10 : 2 * CONSTS + 6] + (inner, inner_back, rims, depth_out)
    (
        conduct,
        neighbours,
        orient,
        depth_spectrum,
        src,
        sent,
        got,
        held_modes,
        extras,
        rim_held,
        base,
        inverse,
        toward_low,
        toward_high,
        margin_low,
        margin_high,
        ends_out,
        ends_in,
        back,
        norm_out,
        norm_x,
        norm_mid,
        src_sem,
        const_sem,
        small_sem,
        go_send,
        go_recv,
        ends_send,
        ends_recv,
        back_send,
        back_recv,
        norm_send,
        norm_recv,
    ) = refs[2 * CONSTS + 6 :]
    depth_in, mu_inner, mu_depth, outer_rows, inner_rows, planes_in, planes_out, mu_planes, mu_rows = consts[:9]

    blk = lax.axis_index("blk")
    py = lax.axis_index("py")
    pz = lax.axis_index("pz")
    place = py * PZ + pz

    def wrapped(a, n):
        return jnp.where(a >= n, a - n, a)

    core = lax.rem(pz, 2)
    chip = pz // 2

    def everyone(visit, first_core):
        def one(near, to_pz):
            to_py = wrapped(py + near, PY)
            visit(to_py, to_pz, to_py * PZ + to_pz)

        def group(turn, carry):
            to_core = turn if first_core == 0 else 1 - turn
            for far in (2, 1, 3):
                for near in (4, 3, 5, 2, 6, 1, 7, 0):
                    one(near, wrapped(chip + far, PZ // 2) * 2 + to_core)
            for near in (4, 3, 5, 2, 6, 1, 7):
                one(near, chip * 2 + to_core)
            return carry

        one(0, chip * 2 + 1 - core)
        lax.fori_loop(0, 2, group, 0)

    barrier = pltpu.get_barrier_semaphore()

    def greet(to_py, to_pz, to):
        pl.semaphore_signal(barrier, inc=1, device_id=(blk, to_py, to_pz), device_id_type=MESH)

    loads = [pltpu.make_async_copy(source.at[y], src.at[y], src_sem.at[y]) for y in range(ROWS)]
    fetches = [pltpu.make_async_copy(a, b, const_sem.at[i]) for i, (a, b) in enumerate(zip(consts_hbm, consts))]
    smalls = [
        pltpu.make_async_copy(a, b, small_sem.at[i])
        for i, (a, b) in enumerate(
            (
                (conduct_hbm, conduct),
                (neighbours_hbm, neighbours),
                (orient_hbm, orient),
                (spectrum_hbm, depth_spectrum),
            )
        )
    ]
    early = fetches[:EARLY] + fetches[9:11]
    late = fetches[EARLY:9] + fetches[11:]
    everyone(greet, 0)
    for start in smalls + loads + early:
        start.start()
    for step in range(1, BLOCKS):
        pl.semaphore_signal(
            barrier, inc=1, device_id=(wrapped(blk + step, BLOCKS), py, pz), device_id_type=MESH
        )
    for fetch in late:
        fetch.start()

    fetches[0].wait()
    squares = jnp.zeros((8, 128), F32)
    rows = []
    for y in range(ROWS):
        loads[y].wait()
        cells = src[y]
        squares = squares + jnp.sum((cells * cells).reshape(BX // 8, 8, NZ), axis=0)
        hi, lo = split(cells)
        rows.append(dot(depth_in[...], jnp.concatenate([hi, lo, hi], axis=1), NT))
    own_squares = jnp.sum(jnp.sum(squares, axis=0, keepdims=True), axis=1, keepdims=True)

    for wait in smalls + early[1:]:
        wait.wait()
    c0 = conduct[0]
    c1 = conduct[1]
    c2 = conduct[2]

    base_part = c0 * mu_inner[...] + c2 * jnp.concatenate([mu_depth[...]] * 2, axis=1)
    weights = jnp.concatenate([0.5 / (base_part + c1), 0.5 / (base_part + 3.0 * c1)], axis=0)
    mixed = jnp.concatenate([rows[1] + rows[2], rows[1] - rows[2]], axis=0)
    inner_modes = times_right(mixed, (inner[0], inner[1]), NN) * weights
    for h in range(HALVES):
        own = [slice(NZ * q + PLANE * h, NZ * q + PLANE * (h + 1)) for q in range(2)]
        weight = jnp.concatenate([weights[part] for part in own], axis=0)
        local[h] = jnp.concatenate([inner_modes[part] for part in own], axis=0)
        by_row[h] = weight * c1
        by_plane[h] = weight * c0
    both = times_right(inner_modes, (inner_back[0], inner_back[1]), NN)
    solved_rows = (both[:NZ] + both[NZ:], both[:NZ] - both[NZ:])
    lanes = lax.broadcasted_iota(jnp.int32, (NZ, 128), 1)
    rim = jnp.zeros((NZ, 128), F32)
    for r in range(2):
        near, far = solved_rows[r][:, :128], solved_rows[r][:, 128:]
        at_first = rows[1 + r][:, :128] + c0 * pltpu.roll(near, 127, 1)
        at_last = rows[1 + r][:, 128:] + c0 * pltpu.roll(far, 1, 1)
        part = jnp.where(lanes == 0, at_first, 0.0)
        part = jnp.where(lanes == 127, at_last, part)
        part = jnp.where(lanes == OV, near, part)
        part = jnp.where(lanes == OV - 1, far, part)
        rim = rim + (part if r == 0 else pltpu.roll(part, 2, 1))
    outer_cells = (rows[0] + c1 * solved_rows[0], rows[3] + c1 * solved_rows[1])
    for h in range(HALVES):
        part = slice(PLANE * h, PLANE * (h + 1))
        for r in range(2):
            for x in range(2):
                sent[h, pl.ds(2 * r + x, PLANE, stride=THERE[h]), :] = outer_cells[r][
                    part, 128 * x : 128 * (x + 1)
                ]
    sent[0, pl.ds(4, PLANE, stride=THERE[0]), :] = rim[:PLANE] + pltpu.roll(rim[PLANE:], 4, 1)

    pl.semaphore_wait(barrier, PLANE - 1 + BLOCKS - 1)

    def exchange(src_ref, dst_ref, send_sem, recv_sem, h, slots, first_core):
        def tile(d):
            return pl.ds(d * slots, slots)

        def send(to_py, to_pz, to):
            pltpu.make_async_remote_copy(
                src_ref=src_ref.at[h, tile(to), :],
                dst_ref=dst_ref.at[h, tile(place), :],
                send_sem=send_sem.at[h],
                recv_sem=recv_sem.at[h],
                device_id=(blk, to_py, to_pz),
                device_id_type=MESH,
            ).start()

        everyone(send, first_core)
        dst_ref[h, tile(place), :] = src_ref[h, tile(place), :]

    def all_of(src_ref, dst_ref, send_sem, recv_sem, h, slots):
        others = pl.ds(0, (PLANE - 1) * slots)
        return pltpu.make_async_remote_copy(
            src_ref=src_ref.at[h, others, :],
            dst_ref=dst_ref.at[h, others, :],
            send_sem=send_sem.at[h],
            recv_sem=recv_sem.at[h],
            device_id=(blk, wrapped(py + 1, PY), pz),
            device_id_type=MESH,
        )

    for h in range(HALVES):
        exchange(sent, got, go_send, go_recv, h, THERE[h], 0)

    for fetch in late:
        fetch.wait()

    order = [jnp.int32(0)]
    for b in range(BLOCKS):
        order[0] = order[0] + b * (neighbours[0, b] == -1).astype(jnp.int32)
    for m in range(1, BLOCKS):
        following = jnp.int32(0)
        for b in range(BLOCKS):
            following = following + neighbours[1, b] * (order[m - 1] == b).astype(jnp.int32)
        order.append(following)
    is_at = [[(order[m] == b).astype(F32) for b in range(BLOCKS)] for m in range(BLOCKS)]
    own_at = [(order[m] == blk).astype(F32) for m in range(BLOCKS)]
    block_flips = [(orient[b] == 1).astype(F32) for b in range(BLOCKS)]
    flips = [sum(is_at[m][b] * block_flips[b] for b in range(BLOCKS)) for m in range(BLOCKS)]
    own_flip = sum(own_at[m] * flips[m] for m in range(BLOCKS))

    row_id = lax.broadcasted_iota(jnp.int32, (8, MODES), 0)

    def pick(flag, yes, no):
        return yes * flag + no * (1.0 - flag)

    plane_id = lax.broadcasted_iota(jnp.int32, (BX, MODES), 0).astype(F32)
    margin_id = lax.broadcasted_iota(jnp.int32, (OV, MODES), 0).astype(F32)
    greens = []
    for h in range(HALVES):
        shift = c1 * mu_rows[...] + c2 * depth_spectrum[PLANE * h + place]
        inverse[h] = 1.0 / (c0 * jnp.concatenate([mu_planes[...]] * 2, axis=1) + shift)
        half = jnp.sqrt(shift / (4.0 * c0))
        square = half * half
        theta = 2.0 * jnp.log1p(half + square / (1.0 + jnp.sqrt(1.0 + square)))

        def power(n):
            return jnp.exp(-n * theta)

        def fall(n):
            return 1.0 - power(2.0 * n)

        scale = 1.0 / (fall(1.0) * fall(385.0))
        f64, f65, f320, f321 = fall(64.0), fall(65.0), fall(320.0), fall(321.0)
        table = {
            (0, 0): power(1.0) * f64 * f321 * scale,
            (0, 1): power(2.0) * f64 * f320 * scale,
            (0, 2): power(257.0) * f64 * f65 * scale,
            (0, 3): power(258.0) * f64 * f64 * scale,
            (1, 1): power(1.0) * f65 * f320 * scale,
            (1, 2): power(256.0) * f65 * f65 * scale,
        }
        for a, b, c, d in ((1, 3, 0, 2), (2, 2, 1, 1), (2, 3, 0, 1), (3, 3, 0, 0)):
            table[a, b] = table[c, d]
        for a in range(4):
            for b in range(a):
                table[a, b] = table[b, a]
        greens.append((table, jnp.exp(theta) * f65 / f64))
        rise = jnp.exp(-plane_id * theta)
        drop = jnp.exp((plane_id - float(BX)) * theta)
        edge = f64 * scale
        far_low = drop * power(64.0)
        far_high = rise * power(65.0)
        toward_low[h] = rise * (power(2.0) * edge) * (1.0 - far_low * far_low)
        toward_high[h] = drop * (power(1.0) * edge) * (1.0 - far_high * far_high)
        inside = jnp.exp((margin_id - float(OV)) * theta)
        margin_low[h] = jnp.exp(-margin_id * theta) * ((1.0 - inside * inside) / f64)
        outside = jnp.exp(-(margin_id + 1.0) * theta)
        margin_high[h] = jnp.exp((margin_id - float(OV - 1)) * theta) * ((1.0 - outside * outside) / f64)

    def to_ends(h, step):
        return pltpu.make_async_remote_copy(
            src_ref=ends_out.at[h],
            dst_ref=ends_in.at[h, blk],
            send_sem=ends_send.at[h, step - 1],
            recv_sem=ends_recv.at[h, step - 1],
            device_id=(wrapped(blk + step, BLOCKS), py, pz),
            device_id_type=MESH,
        )

    def summed(x):
        return jnp.sum(x, axis=0, keepdims=True)

    lane = lax.broadcasted_iota(jnp.int32, (1, 128), 1)

    def total(x):
        return jnp.sum(x, axis=1, keepdims=True)

    def norm_copy(src_ref, dst_ref, stage, step):
        device = (blk, py, wrapped(pz + step, PZ)) if stage == 0 else (blk, wrapped(py + step, PY), pz)
        return pltpu.make_async_remote_copy(
            src_ref=src_ref,
            dst_ref=dst_ref.at[pz if stage == 0 else py],
            send_sem=norm_send.at[stage, step - 1],
            recv_sem=norm_recv.at[stage, step - 1],
            device_id=device,
            device_id_type=MESH,
        )

    change_1 = jnp.zeros((1, MODES), F32)
    change_2 = jnp.zeros((1, MODES), F32)
    total_squares = jnp.zeros((1, 1), F32)
    zero = jnp.zeros((1, MODES), F32)
    def leave_ends(h):
        all_of(sent, got, go_send, go_recv, h, THERE[h]).wait_recv()
        plane = jnp.concatenate([outer_row(got, h, r, THERE[h]) for r in range(2)], axis=0)
        held = times_right(plane.T, (outer_rows[0], outer_rows[1]), NN)
        if h == 0:
            extra = times_right(row_of(got, 0, 4, THERE[0]).T, (inner_rows[0], inner_rows[1]), NN)
            for half in range(HALVES):
                for i, lane_of in enumerate((0, 127, OV, OV - 1)):
                    a, b = (lane_of + 4 * half) % 128, (lane_of + 4 * half + 2) % 128
                    extras[half, i : i + 1, :] = extra[a : a + 1, :MODES] + extra[b : b + 1, MODES:]
        at_first = extras[h, 0:1, :]
        at_last = extras[h, 1:2, :]
        cut_low = extras[h, 2:3, :] * c0
        cut_high = extras[h, 3:4, :] * c0
        held = jnp.concatenate(
            [
                held[:8] + jnp.where(row_id == 0, at_first, 0.0),
                held[8:-8],
                held[-8:] + jnp.where(row_id == 7, at_last, 0.0),
            ],
            axis=0,
        )
        near = (
            jnp.where(row_id == 0, summed(held * toward_low[h]) * (1.0 / c0), 0.0)
            + jnp.where(row_id == 1, summed(held * toward_high[h]) * (1.0 / c0), 0.0)
            + jnp.where(row_id == 2, (summed(held[:OV] * margin_low[h]) - cut_low * margin_low[h, OV - 1 : OV, :]) * (1.0 / c0), 0.0)
            + jnp.where(row_id == 3, (summed(held[BX - OV :] * margin_high[h]) - cut_high * margin_high[h, 0:1, :]) * (1.0 / c0), 0.0)
            + jnp.where(row_id == 4, own_squares, 0.0)
        )
        ends_out[h] = near
        ends_in[h, blk] = near
        for step in range(1, BLOCKS):
            to_ends(h, step).start()

        held_modes[h] = held

    def solve_own(h):
        solved_modes = times((planes_in[0], planes_in[1]), held_modes[h], NN) * inverse[h]
        base[h] = times((planes_out[0], planes_out[1]), solved_modes, NN)

    def give_back(h, total_squares, change_1, change_2):
        table, ratio = greens[h]
        for step in range(1, BLOCKS):
            to_ends(h, step).wait_recv()
        tiles = [ends_in[h, b] for b in range(BLOCKS)]
        if h == 0:
            for b in range(BLOCKS):
                total_squares = total_squares + tiles[b][4:5, :1]
        first, low, high = [], [], []
        for m in range(BLOCKS):
            at = sum(tiles[b] * is_at[m][b] for b in range(BLOCKS))
            left = pick(flips[m], at[1:2], at[0:1])
            right = pick(flips[m], at[0:1], at[1:2])
            first.append([left, left * ratio, right * ratio, right])
            low.append(pick(flips[m], at[3:4], at[2:3]))
            high.append(pick(flips[m], at[2:3], at[3:4]))
        outer = [
            [high[m - 1] if m > 0 else zero, zero, zero, low[m + 1] if m < BLOCKS - 1 else zero]
            for m in range(BLOCKS)
        ]

        def solved(m, p, sources):
            return first[m][p] + sum(table[p, q] * sources[m][q] for q in range(4))

        def jumps(sources):
            last = BLOCKS - 1
            left = [solved(m + 1, 1, sources) - solved(m, 3, sources) for m in range(last)]
            left.append(-solved(last, 3, sources))
            right = [solved(m, 2, sources) - solved(m + 1, 0, sources) for m in range(last)]
            right.append(-solved(0, 0, sources))
            return left, right

        def with_jumps(left, right):
            result = [list(o) for o in outer]
            for m in range(BLOCKS - 1):
                result[m][2] = left[m]
                result[m][3] = outer[m][3] + right[m]
                result[m + 1][1] = right[m]
                result[m + 1][0] = outer[m + 1][0] + left[m]
            result[BLOCKS - 1][2] = left[BLOCKS - 1]
            result[0][1] = right[BLOCKS - 1]
            return result

        left_1, right_1 = jumps(outer)
        left_2, right_2 = jumps(with_jumps(left_1, right_1))
        for a, b in zip(left_1 + right_1, left_2 + right_2):
            change_1 = change_1 + a * a
            change_2 = change_2 + (b - a) * (b - a)
        final = with_jumps(left_2, right_2)
        at_low = sum(own_at[m] * (final[m][0] + ratio * final[m][1]) for m in range(BLOCKS))
        at_high = sum(own_at[m] * (final[m][3] + ratio * final[m][2]) for m in range(BLOCKS))
        at_low, at_high = pick(own_flip, at_high, at_low), pick(own_flip, at_low, at_high)

        if h == HALVES - 1:
            partial = (
                jnp.where(lane == 0, total_squares, 0.0)
                + jnp.where(lane == 1, total(change_1) * (c0 * c0), 0.0)
                + jnp.where(lane == 2, total(change_2) * (c0 * c0), 0.0)
            )
            norm_out[...] = partial
            norm_x[pz] = partial
            for step in range(1, PZ):
                norm_copy(norm_out, norm_x, 0, step).start()

        across = base[h] + toward_low[h] * at_low + toward_high[h] * at_high
        plane = times((outer_rows[0], outer_rows[1]), across, NT)
        ends = [across[:1], across[-1:]]
        edge_modes = jnp.concatenate(
            [
                sum(jnp.where(row_id == 4 * h + 2 * r + e, ends[e], 0.0) for e in range(2))
                for r in range(2)
            ],
            axis=1,
        )
        for r in range(2):
            for x in range(2):
                back[h, pl.ds(2 * r + x, PLANE, stride=BACK[h]), :] = plane[
                    PLANE * r : PLANE * (r + 1), 128 * x : 128 * (x + 1)
                ]
        if h == 0:
            rim_held[...] = edge_modes
        else:
            rim_modes = jnp.concatenate([rim_held[...] + edge_modes, jnp.zeros((120, 2 * MODES), F32)], axis=0)
            back[h, pl.ds(4, PLANE, stride=BACK[h]), :] = times((inner_rows[0], inner_rows[1]), rim_modes, NT)
        exchange(back, returned, back_send, back_recv, h, BACK[h], 1)
        return total_squares, change_1, change_2

    sums = (total_squares, change_1, change_2)
    leave_ends(0)
    solve_own(0)
    leave_ends(1)
    sums = give_back(0, *sums)
    solve_own(1)
    give_back(1, *sums)

    for step in range(1, PZ):
        norm_copy(norm_out, norm_x, 0, step).wait_recv()
    partial = sum(norm_x[i] for i in range(PZ))
    norm_mid[...] = partial
    norm_z[py] = partial
    for step in range(1, PY):
        norm_copy(norm_mid, norm_z, 1, step).start()

    all_of(back, returned, back_send, back_recv, 0, BACK[0]).wait_recv()
    partial_out[0], partial_out[3], mixed = outer_restored(returned, 0, depth_out)
    from_rows = times_right(mixed, (inner[0], inner[1]), NN)
    both = times_right(local[0] + by_row[0] * from_rows, (inner_back[0], inner_back[1]), NN)
    for r, cells in enumerate(rows_of(both)):
        partial_out[1 + r] = depth_back(cells, depth_out[0])

    for h in range(HALVES):
        all_of(sent, got, go_send, go_recv, h, THERE[h]).wait_send()
        for step in range(1, BLOCKS):
            to_ends(h, step).wait_send()
    for step in range(1, PZ):
        norm_copy(norm_out, norm_x, 0, step).wait_send()
    all_of(back, returned, back_send, back_recv, 0, BACK[0]).wait_send()
    all_of(back, returned, back_send, back_recv, 1, BACK[1]).wait_recv()
    for step in range(1, PY):
        norm_copy(norm_mid, norm_z, 1, step).wait_recv()
    all_of(back, returned, back_send, back_recv, 1, BACK[1]).wait_send()
    for step in range(1, PY):
        norm_copy(norm_mid, norm_z, 1, step).wait_send()


def finish(returned, partial_out, norm_z, *refs):
    held, (out, norms, result, roots, out_sem, norm_sem) = refs[:-6], refs[-6:]
    lane = lax.broadcasted_iota(jnp.int32, (1, 128), 1)
    root = jnp.sqrt(sum(norm_z[i] for i in range(PY)) / CELLS)
    for i in range(3):
        roots[i] = jnp.sum(jnp.where(lane == i, root, 0.0))
    copies = [pltpu.make_async_copy(roots, norms, norm_sem)]
    copies[0].start()

    def put(r, cells):
        result[r] = partial_out[r] + cells
        copies.append(pltpu.make_async_copy(result.at[r], out.at[r], out_sem.at[r]))
        copies[-1].start()

    local, by_row, by_plane, inner, inner_back, rims, depth_out = held
    low_cells, high_cells, mixed = outer_restored(returned, 1, depth_out)
    put(0, low_cells)
    put(3, high_cells)
    rim = row_of(returned, 1, 4, BACK[1])[:, :8]
    from_rim = times_right(rim, (rims[0], rims[1]), NN)
    parts = [from_rim[:, BX * q : BX * (q + 1)] for q in range(4)]
    from_rim = [jnp.concatenate(parts[2 * h : 2 * h + 2], axis=0) for h in range(HALVES)]
    from_rows = times_right(mixed, (inner[0], inner[1]), NN)
    second = local[1] + by_row[1] * from_rows + by_plane[1] * from_rim[1]
    both = times_right(
        jnp.concatenate([by_plane[0] * from_rim[0], second], axis=0), (inner_back[0], inner_back[1]), NN
    )
    plane = lax.broadcasted_iota(jnp.int32, (PLANE, BX), 1)
    halves_of = [rows_of(both[2 * PLANE * h : 2 * PLANE * (h + 1)]) for h in range(HALVES)]
    for r in range(2):
        total = None
        for h in range(HALVES):
            slot = 4 * h + 2 * r
            cells = jnp.where(plane == 0, rim[:, slot : slot + 1], halves_of[h][r])
            cells = jnp.where(plane == BX - 1, rim[:, slot + 1 : slot + 2], cells)
            cells = depth_back(cells, depth_out[h])
            total = cells if total is None else total + cells
        put(1 + r, total)
    for copy in copies:
        copy.wait()


def shards(source, conduct, neighbours, orient):
    consts = tables()
    any_space = pl.BlockSpec(memory_space=pltpu.HBM)
    vmem = pl.BlockSpec(memory_space=pltpu.VMEM)
    dma = pltpu.SemaphoreType.DMA
    chunked = (HALVES, PLANE * max(BACK), 128)
    modal = (HALVES, 2 * PLANE, BX)
    cells = pltpu.VMEM((ROWS, BX, NZ), F32)
    limit = 24 * 1024 * 1024
    handed = pl.pallas_call(
        kernel,
        name="schwarz",
        out_shape=(
            jax.ShapeDtypeStruct(chunked, F32),
            jax.ShapeDtypeStruct((ROWS, BX, NZ), F32),
            jax.ShapeDtypeStruct((PY, 1, 128), F32),
            jax.ShapeDtypeStruct(modal, F32),
            jax.ShapeDtypeStruct(modal, F32),
            jax.ShapeDtypeStruct(modal, F32),
            *[jax.ShapeDtypeStruct(c.shape, BF16) for c in consts[-4:]],
        ),
        in_specs=[any_space] * (5 + len(consts)),
        out_specs=(vmem,) * 10,
        scratch_shapes=[pltpu.VMEM(c.shape, c.dtype) for c in consts[:-4]]
        + [
            pltpu.SMEM((3,), F32),
            pltpu.SMEM((2, BLOCKS), jnp.int32),
            pltpu.SMEM((BLOCKS,), jnp.int32),
            pltpu.SMEM((NZ,), F32),
            cells,
            pltpu.VMEM(chunked, F32),
            pltpu.VMEM(chunked, F32),
            pltpu.VMEM((HALVES, BX, MODES), F32),
            pltpu.VMEM((HALVES, 8, MODES), F32),
            pltpu.VMEM((8, 2 * MODES), F32),
            pltpu.VMEM((HALVES, BX, MODES), F32),
            pltpu.VMEM((HALVES, EXT, MODES), F32),
            pltpu.VMEM((HALVES, BX, MODES), F32),
            pltpu.VMEM((HALVES, BX, MODES), F32),
            pltpu.VMEM((HALVES, OV, MODES), F32),
            pltpu.VMEM((HALVES, OV, MODES), F32),
            pltpu.VMEM((HALVES, 8, MODES), F32),
            pltpu.VMEM((HALVES, BLOCKS, 8, MODES), F32),
            pltpu.VMEM(chunked, F32),
            pltpu.VMEM((1, 128), F32),
            pltpu.VMEM((PZ, 1, 128), F32),
            pltpu.VMEM((1, 128), F32),
            dma((ROWS,)),
            dma((len(consts),)),
            dma((4,)),
            dma((HALVES,)),
            dma((HALVES,)),
            dma((HALVES, BLOCKS - 1)),
            dma((HALVES, BLOCKS - 1)),
            dma((HALVES,)),
            dma((HALVES,)),
            dma((2, PZ - 1)),
            dma((2, PZ - 1)),
        ],
        compiler_params=pltpu.CompilerParams(collective_id=0, has_side_effects=True, vmem_limit_bytes=limit),
    )(
        *[
            pltpu.with_memory_space_constraint(jnp.asarray(a), pltpu.HBM)
            for a in (
                source,
                conduct,
                neighbours.T,
                orient,
                eigenvalues(NZ).astype(np.float32),
                *consts,
            )
        ]
    )
    return pl.pallas_call(
        finish,
        name="finish",
        out_shape=(
            jax.ShapeDtypeStruct((ROWS, BX, NZ), F32),
            jax.ShapeDtypeStruct((3,), F32),
        ),
        in_specs=[vmem] * 10,
        out_specs=(any_space, any_space),
        scratch_shapes=[cells, pltpu.SMEM((3,), F32), dma((ROWS,)), dma],
        compiler_params=pltpu.CompilerParams(vmem_limit_bytes=limit),
    )(*handed)


def solution(mesh):
    cells = P(("py", "pz"), "blk", None)
    return jax.shard_map(
        shards, mesh=mesh, in_specs=(cells, P(), P(), P()), out_specs=(cells, P()), check_vma=False
    )
```

```python
import functools

import jax
import jax.numpy as jnp
import ml_dtypes
import numpy as np
from jax import lax
from jax.experimental import pallas as pl
from jax.experimental.pallas import tpu as pltpu
from jax.sharding import PartitionSpec as P

NY = 256
NZ = 128
BX = 256
OV = 64
EXT = 384
BLOCKS = 4
PY = 8
PZ = 8
PLANE = PY * PZ
ROWS = NY // PLANE
HALVES = 2
MODES = 256
MESH = pl.DeviceIdType.MESH
F32 = jnp.float32
BF16 = jnp.bfloat16
NN = (((1,), (0,)), ((), ()))
NT = (((1,), (1,)), ((), ()))
CELLS = float(BLOCKS * BX * NY * NZ)
TN = (((0,), (0,)), ((), ()))
BACK = (4, 5)
THERE = (5, 4)
CONSTS = 13
EARLY = 3


def basis(n):
    j = np.arange(1, n + 1)
    m = (j[:, None] * j[None, :]) % (2 * (n + 1))
    return np.sqrt(2.0 / (n + 1)) * np.sin(np.pi * m / (n + 1))


def eigenvalues(n):
    return 4.0 * np.sin(np.pi * np.arange(1, n + 1) / (2.0 * (n + 1))) ** 2


def halves(a):
    a = a.astype(np.float32)
    hi = a.astype(ml_dtypes.bfloat16)
    lo = (a - hi.astype(np.float32)).astype(ml_dtypes.bfloat16)
    return np.stack([hi, lo])


@functools.lru_cache(None)
def tables():
    depth = halves(basis(NZ))
    rows = basis(NY)
    planes = basis(EXT)
    first = ROWS * np.arange(PLANE)
    outer_rows = rows[np.concatenate([first, first + ROWS - 1])]
    inner_rows = np.concatenate([rows[first + 1], rows[first + 2]], axis=1)
    inner = np.zeros((BX, BX))
    inner[1:-1, :-2] = basis(BX - 2)
    mu_inner = np.concatenate([eigenvalues(BX - 2), np.ones(2)])[None, :]
    rims = np.zeros((8, HALVES * 2 * BX))
    for h in range(HALVES):
        columns = slice(2 * BX * h, 2 * BX * (h + 1))
        rims[4 * h : 4 * h + 4, columns] = np.concatenate(
            [np.stack([inner[1], inner[-2]] * 2), np.stack([inner[1], inner[-2], -inner[1], -inner[-2]])], axis=1
        )
    planes_in = planes[OV : OV + BX].T
    depth_in = np.concatenate([depth[0], depth[0], depth[1]], axis=1)
    depth_out = np.stack(
        [
            np.concatenate([part[PLANE * h : PLANE * (h + 1)] for part in (depth[0], depth[0], depth[1])], axis=0)
            for h in range(HALVES)
        ]
    )
    return (
        depth_in,
        mu_inner.astype(np.float32),
        (eigenvalues(NZ)[:, None] * np.ones((1, 128))).astype(np.float32),
        halves(outer_rows),
        halves(inner_rows),
        halves(planes_in),
        halves(planes_in.T),
        (eigenvalues(EXT)[:, None] * np.ones((1, 128))).astype(np.float32),
        eigenvalues(NY)[None, :].astype(np.float32),
        halves(inner),
        halves(inner.T),
        halves(rims),
        depth_out,
    )


def split(x):
    hi = x.astype(BF16)
    return hi, (x - hi.astype(F32)).astype(BF16)


def dot(a, b, dims):
    return lax.dot_general(a, b, dimension_numbers=dims, preferred_element_type=F32)


def times(table, x, dims):
    hi, lo = split(x)
    return dot(table[0], hi, dims) + (dot(table[0], lo, dims) + dot(table[1], hi, dims))


def times_right(x, table, dims):
    hi, lo = split(x)
    return dot(hi, table[0], dims) + (dot(lo, table[0], dims) + dot(hi, table[1], dims))


def row_of(ref, h, slot, slots):
    return ref[h, pl.ds(slot, PLANE, stride=slots), :]


def outer_row(ref, h, r, slots):
    return jnp.concatenate([row_of(ref, h, 2 * r + x, slots) for x in range(2)], axis=1)


def outer_restored(returned, h, depth_out):
    low_row = outer_row(returned, h, 0, BACK[h])
    high_row = outer_row(returned, h, 1, BACK[h])
    mixed = jnp.concatenate([low_row + high_row, low_row - high_row], axis=0)
    return depth_back(low_row, depth_out[h]), depth_back(high_row, depth_out[h]), mixed


def rows_of(both):
    return both[:PLANE] + both[PLANE:], both[:PLANE] - both[PLANE:]


def depth_back(cells, table):
    hi, lo = split(cells)
    return dot(jnp.concatenate([hi, lo, hi], axis=0), table, TN)


def kernel(source, conduct_hbm, neighbours_hbm, orient_hbm, spectrum_hbm, *refs):
    consts_hbm = refs[:CONSTS]
    returned, partial_out, norm_z, local, by_row, by_plane, inner, inner_back, rims, depth_out = refs[
        CONSTS : CONSTS + 10
    ]
    consts = refs[CONSTS + 10 : 2 * CONSTS + 6] + (inner, inner_back, rims, depth_out)
    (
        conduct,
        neighbours,
        orient,
        depth_spectrum,
        src,
        sent,
        got,
        held_modes,
        extras,
        rim_held,
        base,
        inverse,
        toward_low,
        toward_high,
        margin_low,
        margin_high,
        ends_out,
        ends_in,
        back,
        norm_out,
        norm_x,
        norm_mid,
        src_sem,
        const_sem,
        small_sem,
        go_send,
        go_recv,
        ends_send,
        ends_recv,
        back_send,
        back_recv,
        norm_send,
        norm_recv,
    ) = refs[2 * CONSTS + 6 :]
    depth_in, mu_inner, mu_depth, outer_rows, inner_rows, planes_in, planes_out, mu_planes, mu_rows = consts[:9]

    blk = lax.axis_index("blk")
    py = lax.axis_index("py")
    pz = lax.axis_index("pz")
    place = py * PZ + pz

    def wrapped(a, n):
        return jnp.where(a >= n, a - n, a)

    core = lax.rem(pz, 2)
    chip = pz // 2

    def everyone(visit, first_core):
        def one(near, to_pz):
            to_py = wrapped(py + near, PY)
            visit(to_py, to_pz, to_py * PZ + to_pz)

        def group(turn, carry):
            to_core = turn if first_core == 0 else 1 - turn
            for far in (2, 1, 3):
                for near in (4, 3, 5, 2, 6, 1, 7, 0):
                    one(near, wrapped(chip + far, PZ // 2) * 2 + to_core)
            for near in (4, 3, 5, 2, 6, 1, 7):
                one(near, chip * 2 + to_core)
            return carry

        one(0, chip * 2 + 1 - core)
        lax.fori_loop(0, 2, group, 0)

    barrier = pltpu.get_barrier_semaphore()

    def greet(to_py, to_pz, to):
        pl.semaphore_signal(barrier, inc=1, device_id=(blk, to_py, to_pz), device_id_type=MESH)

    loads = [pltpu.make_async_copy(source.at[y], src.at[y], src_sem.at[y]) for y in range(ROWS)]
    fetches = [pltpu.make_async_copy(a, b, const_sem.at[i]) for i, (a, b) in enumerate(zip(consts_hbm, consts))]
    smalls = [
        pltpu.make_async_copy(a, b, small_sem.at[i])
        for i, (a, b) in enumerate(
            (
                (conduct_hbm, conduct),
                (neighbours_hbm, neighbours),
                (orient_hbm, orient),
                (spectrum_hbm, depth_spectrum),
            )
        )
    ]
    early = fetches[:EARLY] + fetches[9:11]
    late = fetches[EARLY:9] + fetches[11:]
    everyone(greet, 0)
    for start in smalls + loads + early:
        start.start()
    for step in range(1, BLOCKS):
        pl.semaphore_signal(
            barrier, inc=1, device_id=(wrapped(blk + step, BLOCKS), py, pz), device_id_type=MESH
        )
    for fetch in late:
        fetch.start()

    fetches[0].wait()
    squares = jnp.zeros((8, 128), F32)
    rows = []
    for y in range(ROWS):
        loads[y].wait()
        cells = src[y]
        squares = squares + jnp.sum((cells * cells).reshape(BX // 8, 8, NZ), axis=0)
        hi, lo = split(cells)
        rows.append(dot(depth_in[...], jnp.concatenate([hi, lo, hi], axis=1), NT))
    own_squares = jnp.sum(jnp.sum(squares, axis=0, keepdims=True), axis=1, keepdims=True)

    for wait in smalls + early[1:]:
        wait.wait()
    c0 = conduct[0]
    c1 = conduct[1]
    c2 = conduct[2]

    base_part = c0 * mu_inner[...] + c2 * jnp.concatenate([mu_depth[...]] * 2, axis=1)
    weights = jnp.concatenate([0.5 / (base_part + c1), 0.5 / (base_part + 3.0 * c1)], axis=0)
    mixed = jnp.concatenate([rows[1] + rows[2], rows[1] - rows[2]], axis=0)
    inner_modes = times_right(mixed, (inner[0], inner[1]), NN) * weights
    for h in range(HALVES):
        own = [slice(NZ * q + PLANE * h, NZ * q + PLANE * (h + 1)) for q in range(2)]
        weight = jnp.concatenate([weights[part] for part in own], axis=0)
        local[h] = jnp.concatenate([inner_modes[part] for part in own], axis=0)
        by_row[h] = weight * c1
        by_plane[h] = weight * c0
    both = times_right(inner_modes, (inner_back[0], inner_back[1]), NN)
    solved_rows = (both[:NZ] + both[NZ:], both[:NZ] - both[NZ:])
    lanes = lax.broadcasted_iota(jnp.int32, (NZ, 128), 1)
    rim = jnp.zeros((NZ, 128), F32)
    for r in range(2):
        near, far = solved_rows[r][:, :128], solved_rows[r][:, 128:]
        at_first = rows[1 + r][:, :128] + c0 * pltpu.roll(near, 127, 1)
        at_last = rows[1 + r][:, 128:] + c0 * pltpu.roll(far, 1, 1)
        part = jnp.where(lanes == 0, at_first, 0.0)
        part = jnp.where(lanes == 127, at_last, part)
        part = jnp.where(lanes == OV, near, part)
        part = jnp.where(lanes == OV - 1, far, part)
        rim = rim + (part if r == 0 else pltpu.roll(part, 2, 1))
    outer_cells = (rows[0] + c1 * solved_rows[0], rows[3] + c1 * solved_rows[1])
    for h in range(HALVES):
        part = slice(PLANE * h, PLANE * (h + 1))
        for r in range(2):
            for x in range(2):
                sent[h, pl.ds(2 * r + x, PLANE, stride=THERE[h]), :] = outer_cells[r][
                    part, 128 * x : 128 * (x + 1)
                ]
    sent[0, pl.ds(4, PLANE, stride=THERE[0]), :] = rim[:PLANE] + pltpu.roll(rim[PLANE:], 4, 1)

    pl.semaphore_wait(barrier, PLANE - 1 + BLOCKS - 1)

    def exchange(src_ref, dst_ref, send_sem, recv_sem, h, slots, first_core):
        def tile(d):
            return pl.ds(d * slots, slots)

        def send(to_py, to_pz, to):
            pltpu.make_async_remote_copy(
                src_ref=src_ref.at[h, tile(to), :],
                dst_ref=dst_ref.at[h, tile(place), :],
                send_sem=send_sem.at[h],
                recv_sem=recv_sem.at[h],
                device_id=(blk, to_py, to_pz),
                device_id_type=MESH,
            ).start()

        everyone(send, first_core)
        dst_ref[h, tile(place), :] = src_ref[h, tile(place), :]

    def all_of(src_ref, dst_ref, send_sem, recv_sem, h, slots):
        others = pl.ds(0, (PLANE - 1) * slots)
        return pltpu.make_async_remote_copy(
            src_ref=src_ref.at[h, others, :],
            dst_ref=dst_ref.at[h, others, :],
            send_sem=send_sem.at[h],
            recv_sem=recv_sem.at[h],
            device_id=(blk, wrapped(py + 1, PY), pz),
            device_id_type=MESH,
        )

    for h in range(HALVES):
        exchange(sent, got, go_send, go_recv, h, THERE[h], 0)

    for fetch in late:
        fetch.wait()

    order = [jnp.int32(0)]
    for b in range(BLOCKS):
        order[0] = order[0] + b * (neighbours[0, b] == -1).astype(jnp.int32)
    for m in range(1, BLOCKS):
        following = jnp.int32(0)
        for b in range(BLOCKS):
            following = following + neighbours[1, b] * (order[m - 1] == b).astype(jnp.int32)
        order.append(following)
    is_at = [[(order[m] == b).astype(F32) for b in range(BLOCKS)] for m in range(BLOCKS)]
    own_at = [(order[m] == blk).astype(F32) for m in range(BLOCKS)]
    block_flips = [(orient[b] == 1).astype(F32) for b in range(BLOCKS)]
    flips = [sum(is_at[m][b] * block_flips[b] for b in range(BLOCKS)) for m in range(BLOCKS)]
    own_flip = sum(own_at[m] * flips[m] for m in range(BLOCKS))

    row_id = lax.broadcasted_iota(jnp.int32, (8, MODES), 0)

    def pick(flag, yes, no):
        return yes * flag + no * (1.0 - flag)

    plane_id = lax.broadcasted_iota(jnp.int32, (BX, MODES), 0).astype(F32)
    margin_id = lax.broadcasted_iota(jnp.int32, (OV, MODES), 0).astype(F32)
    greens = []
    for h in range(HALVES):
        shift = c1 * mu_rows[...] + c2 * depth_spectrum[PLANE * h + place]
        inverse[h] = 1.0 / (c0 * jnp.concatenate([mu_planes[...]] * 2, axis=1) + shift)
        half = jnp.sqrt(shift / (4.0 * c0))
        square = half * half
        theta = 2.0 * jnp.log1p(half + square / (1.0 + jnp.sqrt(1.0 + square)))

        def power(n):
            return jnp.exp(-n * theta)

        def fall(n):
            return 1.0 - power(2.0 * n)

        scale = 1.0 / (fall(1.0) * fall(385.0))
        f64, f65, f320, f321 = fall(64.0), fall(65.0), fall(320.0), fall(321.0)
        table = {
            (0, 0): power(1.0) * f64 * f321 * scale,
            (0, 1): power(2.0) * f64 * f320 * scale,
            (0, 2): power(257.0) * f64 * f65 * scale,
            (0, 3): power(258.0) * f64 * f64 * scale,
            (1, 1): power(1.0) * f65 * f320 * scale,
            (1, 2): power(256.0) * f65 * f65 * scale,
        }
        for a, b, c, d in ((1, 3, 0, 2), (2, 2, 1, 1), (2, 3, 0, 1), (3, 3, 0, 0)):
            table[a, b] = table[c, d]
        for a in range(4):
            for b in range(a):
                table[a, b] = table[b, a]
        greens.append((table, jnp.exp(theta) * f65 / f64))
        rise = jnp.exp(-plane_id * theta)
        drop = jnp.exp((plane_id - float(BX)) * theta)
        edge = f64 * scale
        far_low = drop * power(64.0)
        far_high = rise * power(65.0)
        toward_low[h] = rise * (power(2.0) * edge) * (1.0 - far_low * far_low)
        toward_high[h] = drop * (power(1.0) * edge) * (1.0 - far_high * far_high)
        inside = jnp.exp((margin_id - float(OV)) * theta)
        margin_low[h] = jnp.exp(-margin_id * theta) * ((1.0 - inside * inside) / f64)
        outside = jnp.exp(-(margin_id + 1.0) * theta)
        margin_high[h] = jnp.exp((margin_id - float(OV - 1)) * theta) * ((1.0 - outside * outside) / f64)

    def to_ends(h, step):
        return pltpu.make_async_remote_copy(
            src_ref=ends_out.at[h],
            dst_ref=ends_in.at[h, blk],
            send_sem=ends_send.at[h, step - 1],
            recv_sem=ends_recv.at[h, step - 1],
            device_id=(wrapped(blk + step, BLOCKS), py, pz),
            device_id_type=MESH,
        )

    def summed(x):
        return jnp.sum(x, axis=0, keepdims=True)

    lane = lax.broadcasted_iota(jnp.int32, (1, 128), 1)

    def total(x):
        return jnp.sum(x, axis=1, keepdims=True)

    def norm_copy(src_ref, dst_ref, stage, step):
        device = (blk, py, wrapped(pz + step, PZ)) if stage == 0 else (blk, wrapped(py + step, PY), pz)
        return pltpu.make_async_remote_copy(
            src_ref=src_ref,
            dst_ref=dst_ref.at[pz if stage == 0 else py],
            send_sem=norm_send.at[stage, step - 1],
            recv_sem=norm_recv.at[stage, step - 1],
            device_id=device,
            device_id_type=MESH,
        )

    change_1 = jnp.zeros((1, MODES), F32)
    change_2 = jnp.zeros((1, MODES), F32)
    total_squares = jnp.zeros((1, 1), F32)
    zero = jnp.zeros((1, MODES), F32)
    def leave_ends(h):
        all_of(sent, got, go_send, go_recv, h, THERE[h]).wait_recv()
        plane = jnp.concatenate([outer_row(got, h, r, THERE[h]) for r in range(2)], axis=0)
        held = times_right(plane.T, (outer_rows[0], outer_rows[1]), NN)
        if h == 0:
            extra = times_right(row_of(got, 0, 4, THERE[0]).T, (inner_rows[0], inner_rows[1]), NN)
            for half in range(HALVES):
                for i, lane_of in enumerate((0, 127, OV, OV - 1)):
                    a, b = (lane_of + 4 * half) % 128, (lane_of + 4 * half + 2) % 128
                    extras[half, i : i + 1, :] = extra[a : a + 1, :MODES] + extra[b : b + 1, MODES:]
        at_first = extras[h, 0:1, :]
        at_last = extras[h, 1:2, :]
        cut_low = extras[h, 2:3, :] * c0
        cut_high = extras[h, 3:4, :] * c0
        held = jnp.concatenate(
            [
                held[:8] + jnp.where(row_id == 0, at_first, 0.0),
                held[8:-8],
                held[-8:] + jnp.where(row_id == 7, at_last, 0.0),
            ],
            axis=0,
        )
        near = (
            jnp.where(row_id == 0, summed(held * toward_low[h]) * (1.0 / c0), 0.0)
            + jnp.where(row_id == 1, summed(held * toward_high[h]) * (1.0 / c0), 0.0)
            + jnp.where(row_id == 2, (summed(held[:OV] * margin_low[h]) - cut_low * margin_low[h, OV - 1 : OV, :]) * (1.0 / c0), 0.0)
            + jnp.where(row_id == 3, (summed(held[BX - OV :] * margin_high[h]) - cut_high * margin_high[h, 0:1, :]) * (1.0 / c0), 0.0)
            + jnp.where(row_id == 4, own_squares, 0.0)
        )
        ends_out[h] = near
        ends_in[h, blk] = near
        for step in range(1, BLOCKS):
            to_ends(h, step).start()

        held_modes[h] = held

    def solve_own(h):
        solved_modes = times((planes_in[0], planes_in[1]), held_modes[h], NN) * inverse[h]
        base[h] = times((planes_out[0], planes_out[1]), solved_modes, NN)

    def give_back(h, total_squares, change_1, change_2):
        table, ratio = greens[h]
        for step in range(1, BLOCKS):
            to_ends(h, step).wait_recv()
        tiles = [ends_in[h, b] for b in range(BLOCKS)]
        if h == 0:
            for b in range(BLOCKS):
                total_squares = total_squares + tiles[b][4:5, :1]
        first, low, high = [], [], []
        for m in range(BLOCKS):
            at = sum(tiles[b] * is_at[m][b] for b in range(BLOCKS))
            left = pick(flips[m], at[1:2], at[0:1])
            right = pick(flips[m], at[0:1], at[1:2])
            first.append([left, left * ratio, right * ratio, right])
            low.append(pick(flips[m], at[3:4], at[2:3]))
            high.append(pick(flips[m], at[2:3], at[3:4]))
        outer = [
            [high[m - 1] if m > 0 else zero, zero, zero, low[m + 1] if m < BLOCKS - 1 else zero]
            for m in range(BLOCKS)
        ]

        def solved(m, p, sources):
            return first[m][p] + sum(table[p, q] * sources[m][q] for q in range(4))

        def jumps(sources):
            last = BLOCKS - 1
            left = [solved(m + 1, 1, sources) - solved(m, 3, sources) for m in range(last)]
            left.append(-solved(last, 3, sources))
            right = [solved(m, 2, sources) - solved(m + 1, 0, sources) for m in range(last)]
            right.append(-solved(0, 0, sources))
            return left, right

        def with_jumps(left, right):
            result = [list(o) for o in outer]
            for m in range(BLOCKS - 1):
                result[m][2] = left[m]
                result[m][3] = outer[m][3] + right[m]
                result[m + 1][1] = right[m]
                result[m + 1][0] = outer[m + 1][0] + left[m]
            result[BLOCKS - 1][2] = left[BLOCKS - 1]
            result[0][1] = right[BLOCKS - 1]
            return result

        left_1, right_1 = jumps(outer)
        left_2, right_2 = jumps(with_jumps(left_1, right_1))
        for a, b in zip(left_1 + right_1, left_2 + right_2):
            change_1 = change_1 + a * a
            change_2 = change_2 + (b - a) * (b - a)
        final = with_jumps(left_2, right_2)
        at_low = sum(own_at[m] * (final[m][0] + ratio * final[m][1]) for m in range(BLOCKS))
        at_high = sum(own_at[m] * (final[m][3] + ratio * final[m][2]) for m in range(BLOCKS))
        at_low, at_high = pick(own_flip, at_high, at_low), pick(own_flip, at_low, at_high)

        across = base[h] + toward_low[h] * at_low + toward_high[h] * at_high
        plane = times((outer_rows[0], outer_rows[1]), across, NT)
        ends = [across[:1], across[-1:]]
        edge_modes = jnp.concatenate(
            [
                sum(jnp.where(row_id == 4 * h + 2 * r + e, ends[e], 0.0) for e in range(2))
                for r in range(2)
            ],
            axis=1,
        )
        for r in range(2):
            for x in range(2):
                back[h, pl.ds(2 * r + x, PLANE, stride=BACK[h]), :] = plane[
                    PLANE * r : PLANE * (r + 1), 128 * x : 128 * (x + 1)
                ]
        if h == 0:
            rim_held[...] = edge_modes
        else:
            rim_modes = jnp.concatenate([rim_held[...] + edge_modes, jnp.zeros((120, 2 * MODES), F32)], axis=0)
            back[h, pl.ds(4, PLANE, stride=BACK[h]), :] = times((inner_rows[0], inner_rows[1]), rim_modes, NT)
        if h == HALVES - 1:
            partial = (
                jnp.where(lane == 0, total_squares, 0.0)
                + jnp.where(lane == 1, total(change_1) * (c0 * c0), 0.0)
                + jnp.where(lane == 2, total(change_2) * (c0 * c0), 0.0)
            )
            norm_out[...] = partial
            norm_x[pz] = partial
            for step in range(1, PZ):
                norm_copy(norm_out, norm_x, 0, step).start()

        exchange(back, returned, back_send, back_recv, h, BACK[h], 1)
        return total_squares, change_1, change_2

    sums = (total_squares, change_1, change_2)
    leave_ends(0)
    solve_own(0)
    leave_ends(1)
    sums = give_back(0, *sums)
    solve_own(1)
    give_back(1, *sums)

    for step in range(1, PZ):
        norm_copy(norm_out, norm_x, 0, step).wait_recv()
    partial = sum(norm_x[i] for i in range(PZ))
    norm_mid[...] = partial
    norm_z[py] = partial
    for step in range(1, PY):
        norm_copy(norm_mid, norm_z, 1, step).start()

    all_of(back, returned, back_send, back_recv, 0, BACK[0]).wait_recv()
    partial_out[0], partial_out[3], mixed = outer_restored(returned, 0, depth_out)
    from_rows = times_right(mixed, (inner[0], inner[1]), NN)
    both = times_right(local[0] + by_row[0] * from_rows, (inner_back[0], inner_back[1]), NN)
    for r, cells in enumerate(rows_of(both)):
        partial_out[1 + r] = depth_back(cells, depth_out[0])

    for h in range(HALVES):
        all_of(sent, got, go_send, go_recv, h, THERE[h]).wait_send()
        for step in range(1, BLOCKS):
            to_ends(h, step).wait_send()
    for step in range(1, PZ):
        norm_copy(norm_out, norm_x, 0, step).wait_send()
    all_of(back, returned, back_send, back_recv, 0, BACK[0]).wait_send()
    all_of(back, returned, back_send, back_recv, 1, BACK[1]).wait_recv()
    for step in range(1, PY):
        norm_copy(norm_mid, norm_z, 1, step).wait_recv()
    all_of(back, returned, back_send, back_recv, 1, BACK[1]).wait_send()
    for step in range(1, PY):
        norm_copy(norm_mid, norm_z, 1, step).wait_send()


def finish(returned, partial_out, norm_z, *refs):
    held, (out, norms, result, roots, out_sem, norm_sem) = refs[:-6], refs[-6:]
    lane = lax.broadcasted_iota(jnp.int32, (1, 128), 1)
    root = jnp.sqrt(sum(norm_z[i] for i in range(PY)) / CELLS)
    for i in range(3):
        roots[i] = jnp.sum(jnp.where(lane == i, root, 0.0))
    copies = [pltpu.make_async_copy(roots, norms, norm_sem)]
    copies[0].start()

    def put(r, cells):
        result[r] = partial_out[r] + cells
        copies.append(pltpu.make_async_copy(result.at[r], out.at[r], out_sem.at[r]))
        copies[-1].start()

    local, by_row, by_plane, inner, inner_back, rims, depth_out = held
    low_cells, high_cells, mixed = outer_restored(returned, 1, depth_out)
    put(0, low_cells)
    put(3, high_cells)
    rim = row_of(returned, 1, 4, BACK[1])[:, :8]
    from_rim = times_right(rim, (rims[0], rims[1]), NN)
    parts = [from_rim[:, BX * q : BX * (q + 1)] for q in range(4)]
    from_rim = [jnp.concatenate(parts[2 * h : 2 * h + 2], axis=0) for h in range(HALVES)]
    from_rows = times_right(mixed, (inner[0], inner[1]), NN)
    second = local[1] + by_row[1] * from_rows + by_plane[1] * from_rim[1]
    both = times_right(
        jnp.concatenate([by_plane[0] * from_rim[0], second], axis=0), (inner_back[0], inner_back[1]), NN
    )
    plane = lax.broadcasted_iota(jnp.int32, (PLANE, BX), 1)
    halves_of = [rows_of(both[2 * PLANE * h : 2 * PLANE * (h + 1)]) for h in range(HALVES)]
    for r in range(2):
        total = None
        for h in range(HALVES):
            slot = 4 * h + 2 * r
            cells = jnp.where(plane == 0, rim[:, slot : slot + 1], halves_of[h][r])
            cells = jnp.where(plane == BX - 1, rim[:, slot + 1 : slot + 2], cells)
            cells = depth_back(cells, depth_out[h])
            total = cells if total is None else total + cells
        put(1 + r, total)
    for copy in copies:
        copy.wait()


def shards(source, conduct, neighbours, orient):
    consts = tables()
    any_space = pl.BlockSpec(memory_space=pltpu.HBM)
    vmem = pl.BlockSpec(memory_space=pltpu.VMEM)
    dma = pltpu.SemaphoreType.DMA
    chunked = (HALVES, PLANE * max(BACK), 128)
    modal = (HALVES, 2 * PLANE, BX)
    cells = pltpu.VMEM((ROWS, BX, NZ), F32)
    limit = 24 * 1024 * 1024
    handed = pl.pallas_call(
        kernel,
        name="schwarz",
        out_shape=(
            jax.ShapeDtypeStruct(chunked, F32),
            jax.ShapeDtypeStruct((ROWS, BX, NZ), F32),
            jax.ShapeDtypeStruct((PY, 1, 128), F32),
            jax.ShapeDtypeStruct(modal, F32),
            jax.ShapeDtypeStruct(modal, F32),
            jax.ShapeDtypeStruct(modal, F32),
            *[jax.ShapeDtypeStruct(c.shape, BF16) for c in consts[-4:]],
        ),
        in_specs=[any_space] * (5 + len(consts)),
        out_specs=(vmem,) * 10,
        scratch_shapes=[pltpu.VMEM(c.shape, c.dtype) for c in consts[:-4]]
        + [
            pltpu.SMEM((3,), F32),
            pltpu.SMEM((2, BLOCKS), jnp.int32),
            pltpu.SMEM((BLOCKS,), jnp.int32),
            pltpu.SMEM((NZ,), F32),
            cells,
            pltpu.VMEM(chunked, F32),
            pltpu.VMEM(chunked, F32),
            pltpu.VMEM((HALVES, BX, MODES), F32),
            pltpu.VMEM((HALVES, 8, MODES), F32),
            pltpu.VMEM((8, 2 * MODES), F32),
            pltpu.VMEM((HALVES, BX, MODES), F32),
            pltpu.VMEM((HALVES, EXT, MODES), F32),
            pltpu.VMEM((HALVES, BX, MODES), F32),
            pltpu.VMEM((HALVES, BX, MODES), F32),
            pltpu.VMEM((HALVES, OV, MODES), F32),
            pltpu.VMEM((HALVES, OV, MODES), F32),
            pltpu.VMEM((HALVES, 8, MODES), F32),
            pltpu.VMEM((HALVES, BLOCKS, 8, MODES), F32),
            pltpu.VMEM(chunked, F32),
            pltpu.VMEM((1, 128), F32),
            pltpu.VMEM((PZ, 1, 128), F32),
            pltpu.VMEM((1, 128), F32),
            dma((ROWS,)),
            dma((len(consts),)),
            dma((4,)),
            dma((HALVES,)),
            dma((HALVES,)),
            dma((HALVES, BLOCKS - 1)),
            dma((HALVES, BLOCKS - 1)),
            dma((HALVES,)),
            dma((HALVES,)),
            dma((2, PZ - 1)),
            dma((2, PZ - 1)),
        ],
        compiler_params=pltpu.CompilerParams(collective_id=0, has_side_effects=True, vmem_limit_bytes=limit),
    )(
        *[
            pltpu.with_memory_space_constraint(jnp.asarray(a), pltpu.HBM)
            for a in (
                source,
                conduct,
                neighbours.T,
                orient,
                eigenvalues(NZ).astype(np.float32),
                *consts,
            )
        ]
    )
    return pl.pallas_call(
        finish,
        name="finish",
        out_shape=(
            jax.ShapeDtypeStruct((ROWS, BX, NZ), F32),
            jax.ShapeDtypeStruct((3,), F32),
        ),
        in_specs=[vmem] * 10,
        out_specs=(any_space, any_space),
        scratch_shapes=[cells, pltpu.SMEM((3,), F32), dma((ROWS,)), dma],
        compiler_params=pltpu.CompilerParams(vmem_limit_bytes=limit),
    )(*handed)


def solution(mesh):
    cells = P(("py", "pz"), "blk", None)
    return jax.shard_map(
        shards, mesh=mesh, in_specs=(cells, P(), P(), P()), out_specs=(cells, P()), check_vma=False
    )
```
